32 devices in a mesh: dp: 2 (over x), sub: 4 (over z), ep: 4 (over y, core).
Axes of the slice: x: 2, y: 2, z: 4, core: 2. Of those that a mesh axis runs over, the one named last changes fastest.
Arguments:
- input_a: bfloat16 [32, 256, 2048], P(('dp', 'ep', 'sub')), parts along dimension 0
- input_b: bfloat16 [32, 256, 2048], P(('dp', 'ep', 'sub')), parts along dimension 0
- route_idx: int32 [2, 8192, 8], P(None, ('dp', 'ep', 'sub')), parts along dimension 1
- route_gate: float32 [2, 8192, 8], P(None, ('dp', 'ep', 'sub')), parts along dimension 1
- attn_norm: float32 [2048], replicated
- w_query: bfloat16 [2048, 16, 128], replicated
- w_key: bfloat16 [2048, 16, 128], replicated
- w_value: bfloat16 [2048, 16, 128], replicated
- w_out: bfloat16 [16, 128, 2048], replicated
- moe_norm: float32 [2048], replicated
- w_gate: bfloat16 [64, 2048, 1024], P(('ep', 'sub'))
- w_up: bfloat16 [64, 2048, 1024], P(('ep', 'sub'))
- w_down: bfloat16 [64, 1024, 2048], P(('ep', 'sub'))
Outputs:
- output 1: bfloat16 [32, 256, 2048], P(('dp', 'ep', 'sub')), parts along dimension 0
- output 2: bfloat16 [32, 256, 2048], P(('dp', 'ep', 'sub')), parts along dimension 0
There are 2 independent parts. The reference program is written for one: setup_inputs(seed, part) draws one part's arguments, and reference() takes and returns one part's arrays. A program takes and returns all parts, laid end to end along the dimension named above; an argument that names none is the same for every part.
All inputs are finite; a program needn't handle non-finite values.
Results may differ from the reference program's by a relative error of at most 0.0132676.
Values are sent between devices in bfloat16 or wider.
A program may use at most 1 GiB of HBM per device.

```python
import functools
import jax
import jax.numpy as jnp
from jax import lax

MODEL_DIM = 2048
NUM_HEADS = 16
HEAD_DIM = 128
FF_DIM = 1024
TOP_K = 8
TOK_DEV = 256
SEQ_LEN = 256
EXP_LOCAL = 4
EP_SIZE = 4
SUB_SIZE = 4
NODE_LIM = 2

NUM_DEV = EP_SIZE * SUB_SIZE
NUM_EXP = EXP_LOCAL * NUM_DEV
NUM_TOK = NUM_DEV * TOK_DEV
NUM_SEQ = NUM_TOK // SEQ_LEN
CAP_SLOTS = 3 * TOP_K * TOK_DEV // (2 * NUM_EXP)
EXP_ROOM = NUM_DEV * CAP_SLOTS
NODE_EXP = SUB_SIZE * EXP_LOCAL
PER_VISIT = TOP_K // NODE_LIM
HOT_VISITS = 3 * NODE_LIM * TOK_DEV // (2 * EP_SIZE)
COLD_VISITS = NODE_LIM * TOK_DEV // (2 * EP_SIZE)
NORM_EPS = 1e-6


def draw_device_routes(rng_key):
    key_hot, key_tok, key_exp = jax.random.split(rng_key, 3)
    node_rank = jax.random.permutation(key_hot, jnp.arange(EP_SIZE))
    visits = jnp.where(node_rank < EP_SIZE // 2, HOT_VISITS, COLD_VISITS)
    run_ends = jnp.cumsum(visits)
    run_starts = run_ends - visits
    positions = jnp.arange(NODE_LIM * TOK_DEV)
    node_of = jnp.sum(positions[:, None] >= run_ends[None, :], axis=1)
    within = positions - run_starts[node_of]
    node_visits = visits[node_of]
    copies = node_visits * PER_VISIT // NODE_EXP
    list_pos = jnp.arange(PER_VISIT)[None, :] * node_visits[:, None] + within[:, None]
    local_rank = list_pos // copies[:, None]
    exp_keys = jax.random.split(key_exp, EP_SIZE)
    exp_perm = jax.vmap(jax.random.permutation)(exp_keys, jnp.tile(jnp.arange(NODE_EXP), (EP_SIZE, 1)))
    expert = node_of[:, None] * NODE_EXP + exp_perm[node_of[:, None], local_rank]
    expert = expert.reshape(NODE_LIM, TOK_DEV, PER_VISIT).transpose(1, 0, 2).reshape(TOK_DEV, TOP_K)
    tok_perm = jax.random.permutation(key_tok, jnp.arange(TOK_DEV))
    return expert[tok_perm].astype(jnp.int32)


def setup_inputs(seed: int = 0, part: int = 0) -> dict:
    part_key = jax.random.fold_in(jax.random.key(seed), part)
    part_keys = jax.random.split(part_key, 4)
    tok_shape = (NUM_SEQ, SEQ_LEN, MODEL_DIM)
    input_a = jax.random.normal(part_keys[0], tok_shape, jnp.float32).astype(jnp.bfloat16)
    input_b = jax.random.normal(part_keys[1], tok_shape, jnp.float32).astype(jnp.bfloat16)
    route_keys = jax.random.split(part_keys[2], 2 * NUM_DEV)
    route_idx = jax.vmap(draw_device_routes)(route_keys).reshape(2, NUM_TOK, TOP_K)
    logits = 0.5 * jax.random.normal(part_keys[3], (2, NUM_TOK, TOP_K), jnp.float32)
    route_gate = TOP_K * jax.nn.softmax(logits, axis=-1)
    w_keys = jax.random.split(jax.random.key(seed + 1), 9)
    proj_shape = (MODEL_DIM, NUM_HEADS, HEAD_DIM)
    attn_norm = jax.random.uniform(w_keys[0], (MODEL_DIM,), jnp.float32, 0.5, 1.5)
    w_query = (jax.random.normal(w_keys[1], proj_shape, jnp.float32) * MODEL_DIM ** -0.5).astype(jnp.bfloat16)
    w_key = (jax.random.normal(w_keys[2], proj_shape, jnp.float32) * MODEL_DIM ** -0.5).astype(jnp.bfloat16)
    w_value = (jax.random.normal(w_keys[3], proj_shape, jnp.float32) * MODEL_DIM ** -0.5).astype(jnp.bfloat16)
    w_out = (jax.random.normal(w_keys[4], (NUM_HEADS, HEAD_DIM, MODEL_DIM), jnp.float32) * (2.0 * (NUM_HEADS * HEAD_DIM) ** -0.5)).astype(jnp.bfloat16)
    moe_norm = jax.random.uniform(w_keys[5], (MODEL_DIM,), jnp.float32, 0.5, 1.5)
    w_gate = (jax.random.normal(w_keys[6], (NUM_EXP, MODEL_DIM, FF_DIM), jnp.float32) * MODEL_DIM ** -0.5).astype(jnp.bfloat16)
    w_up = (jax.random.normal(w_keys[7], (NUM_EXP, MODEL_DIM, FF_DIM), jnp.float32) * MODEL_DIM ** -0.5).astype(jnp.bfloat16)
    w_down = (jax.random.normal(w_keys[8], (NUM_EXP, FF_DIM, MODEL_DIM), jnp.float32) * FF_DIM ** -0.5).astype(jnp.bfloat16)
    return {'input_a': input_a, 'input_b': input_b, 'route_idx': route_idx, 'route_gate': route_gate, 'attn_norm': attn_norm, 'w_query': w_query, 'w_key': w_key, 'w_value': w_value, 'w_out': w_out, 'moe_norm': moe_norm, 'w_gate': w_gate, 'w_up': w_up, 'w_down': w_down}


def rms_norm(values, norm_gain):
    acc_f32 = values.astype(jnp.float32)
    inv_rms = lax.rsqrt(jnp.mean(acc_f32 * acc_f32, axis=-1, keepdims=True) + NORM_EPS)
    return (acc_f32 * inv_rms * norm_gain).astype(jnp.bfloat16)


def attention_seq(seq_tok, attn_norm, w_query, w_key, w_value, w_out):
    normed = rms_norm(seq_tok, attn_norm).astype(jnp.float32)
    q_heads = jnp.einsum('sd,dhc->shc', normed, w_query.astype(jnp.float32)).astype(jnp.bfloat16)
    k_heads = jnp.einsum('sd,dhc->shc', normed, w_key.astype(jnp.float32)).astype(jnp.bfloat16)
    v_heads = jnp.einsum('sd,dhc->shc', normed, w_value.astype(jnp.float32)).astype(jnp.bfloat16)
    scores = jnp.einsum('qhc,khc->hqk', q_heads.astype(jnp.float32), k_heads.astype(jnp.float32)) * HEAD_DIM ** -0.5
    causal = jnp.arange(SEQ_LEN)[:, None] >= jnp.arange(SEQ_LEN)[None, :]
    scores = jnp.where(causal[None, :, :], scores, -jnp.inf)
    prob_bf = jax.nn.softmax(scores, axis=-1).astype(jnp.bfloat16)
    context = jnp.einsum('hqk,khc->qhc', prob_bf.astype(jnp.float32), v_heads.astype(jnp.float32)).astype(jnp.bfloat16)
    proj_out = jnp.einsum('qhc,hcd->qd', context.astype(jnp.float32), w_out.astype(jnp.float32))
    return (seq_tok.astype(jnp.float32) + proj_out).astype(jnp.bfloat16)


def expert_apply(operands):
    expert_rows, gate_mat, up_mat, down_mat = operands
    gate_h = jnp.dot(expert_rows, gate_mat, preferred_element_type=jnp.float32)
    up_h = jnp.dot(expert_rows, up_mat, preferred_element_type=jnp.float32)
    act_rows = (jax.nn.silu(gate_h) * up_h).astype(jnp.bfloat16)
    return jnp.dot(act_rows, down_mat, preferred_element_type=jnp.float32).astype(jnp.bfloat16)


def moe_layer(hidden, exp_ids, gate_w, moe_norm, w_gate, w_up, w_down):
    normed = rms_norm(hidden, moe_norm)
    flat_ids = exp_ids.reshape(-1)
    sort_order = jnp.argsort(flat_ids, stable=True)
    sorted_ids = flat_ids[sort_order]
    counts = jnp.bincount(flat_ids, length=NUM_EXP)
    starts = jnp.cumsum(counts) - counts
    slot_rank = jnp.arange(NUM_TOK * TOP_K) - starts[sorted_ids]
    slot_sorted = sorted_ids * EXP_ROOM + slot_rank
    holder = jnp.full((NUM_EXP * EXP_ROOM,), NUM_TOK, jnp.int32).at[slot_sorted].set(sort_order // TOP_K)
    disp_rows = jnp.take(normed, holder, axis=0, mode='fill', fill_value=0).reshape(NUM_EXP, EXP_ROOM, MODEL_DIM)
    expert_out = lax.map(expert_apply, (disp_rows, w_gate, w_up, w_down))
    slot_of = jnp.zeros_like(flat_ids).at[sort_order].set(slot_sorted)
    picked = jnp.take(expert_out.reshape(NUM_EXP * EXP_ROOM, MODEL_DIM), slot_of, axis=0).reshape(NUM_TOK, TOP_K, MODEL_DIM)
    moe_sum = jnp.sum(gate_w[:, :, None] * picked.astype(jnp.float32), axis=1)
    return (hidden.astype(jnp.float32) + moe_sum).astype(jnp.bfloat16)


def reference(input_a, input_b, route_idx, route_gate, attn_norm, w_query, w_key, w_value, w_out, moe_norm, w_gate, w_up, w_down):
    attend = functools.partial(attention_seq, attn_norm=attn_norm, w_query=w_query, w_key=w_key, w_value=w_value, w_out=w_out)

    def micro_pass(tokens, exp_ids, gate_w):
        hidden = lax.map(attend, tokens).reshape(NUM_TOK, MODEL_DIM)
        mixed_out = moe_layer(hidden, exp_ids, gate_w, moe_norm, w_gate, w_up, w_down)
        return mixed_out.reshape(NUM_SEQ, SEQ_LEN, MODEL_DIM)

    return micro_pass(input_a, route_idx[0], route_gate[0]), micro_pass(input_b, route_idx[1], route_gate[1])
```

```python
import functools

import jax
import jax.numpy as jnp
from jax import lax
from jax.experimental import pallas as pl
from jax.experimental.pallas import tpu as pltpu
from jax.sharding import PartitionSpec as P

NORM_EPS = 1e-6
MESH = pl.DeviceIdType.MESH
VMEM_CAP = 60 * 1024 * 1024


def rms_norm(values, norm_gain):
    acc_f32 = values.astype(jnp.float32)
    inv_rms = lax.rsqrt(jnp.mean(acc_f32 * acc_f32, axis=-1, keepdims=True) + NORM_EPS)
    return (acc_f32 * inv_rms * norm_gain).astype(jnp.bfloat16)


def attention_block(tokens, attn_norm, w_query, w_key, w_value, w_out):
    normed = rms_norm(tokens, attn_norm)
    q_heads = jnp.einsum('bsd,dhc->bshc', normed, w_query, preferred_element_type=jnp.float32).astype(jnp.bfloat16)
    k_heads = jnp.einsum('bsd,dhc->bshc', normed, w_key, preferred_element_type=jnp.float32).astype(jnp.bfloat16)
    v_heads = jnp.einsum('bsd,dhc->bshc', normed, w_value, preferred_element_type=jnp.float32).astype(jnp.bfloat16)
    score_scale = w_query.shape[2] ** -0.5
    scores = jnp.einsum('bqhc,bkhc->bhqk', q_heads, k_heads, preferred_element_type=jnp.float32) * score_scale
    seq_len = tokens.shape[1]
    causal = lax.broadcasted_iota(jnp.int32, (seq_len, seq_len), 0) >= lax.broadcasted_iota(jnp.int32, (seq_len, seq_len), 1)
    scores = jnp.where(causal, scores, -jnp.inf)
    prob_bf = jax.nn.softmax(scores, axis=-1).astype(jnp.bfloat16)
    context = jnp.einsum('bhqk,bkhc->bqhc', prob_bf, v_heads, preferred_element_type=jnp.float32).astype(jnp.bfloat16)
    proj_out = jnp.einsum('crid,ide->cre', context, w_out, preferred_element_type=jnp.float32)
    return (tokens.astype(jnp.float32) + proj_out).astype(jnp.bfloat16)


def slot_codes(exp_ids, num_exp, cap_slots):
    hits = exp_ids[:, :, None] == jnp.arange(num_exp, dtype=jnp.int32)[None, None, :]
    chosen = jnp.any(hits, axis=1)
    tok_count = exp_ids.shape[0]
    before = lax.broadcasted_iota(jnp.int32, (tok_count, tok_count), 0) > lax.broadcasted_iota(jnp.int32, (tok_count, tok_count), 1)
    rank = jnp.dot(before.astype(jnp.bfloat16), chosen.astype(jnp.bfloat16), preferred_element_type=jnp.float32)
    rank_of = jnp.sum(jnp.where(hits, rank[:, None, :], 0.0), axis=2)
    return exp_ids.astype(jnp.float32) * cap_slots + rank_of


def greet(sub, sub_size, peers, to_left, to_right):
    barrier = pltpu.get_barrier_semaphore()
    last = sub_size - 1

    def hello(dev):
        pl.semaphore_signal(barrier, inc=1, device_id=dev, device_id_type=MESH)

    for dev in peers:
        hello(dev)
    pl.when(sub > 0)(lambda: hello(to_left))
    pl.when(sub < last)(lambda: hello(to_right))
    pl.semaphore_wait(barrier, len(peers) + (sub + last) // sub_size + (2 * last - sub) // sub_size)


def gather_body(count, sub_size, *refs):
    ins, outs = refs[:count], refs[count:2 * count]
    stage = refs[2 * count:3 * count]
    recv, right_s, left_s, far_s, core_s, loc = refs[3 * count:]
    ep, sub = lax.axis_index('ep'), lax.axis_index('sub')
    ep_far = lax.rem(ep + 2, 4)
    ep_core = ep + 1 - 2 * lax.rem(ep, 2)
    ep_diag = lax.rem(ep_core + 2, 4)
    last = sub_size - 1
    to_right, to_left = {'ep': ep, 'sub': sub + 1}, {'ep': ep, 'sub': sub - 1}
    to_far, to_core = {'ep': ep_far, 'sub': sub}, {'ep': ep_core, 'sub': sub}
    greet(sub, sub_size, [to_far, to_core], to_left, to_right)

    def copies(src, blk, sem, slot, dev):
        return [pltpu.make_async_remote_copy(src_ref=src(a), dst_ref=outs[a].at[blk], send_sem=sem.at[a, slot], recv_sem=recv.at[a, blk], device_id=dev, device_id_type=MESH) for a in range(count)]

    def start(*args):
        for cp in copies(*args):
            cp.start()

    def landed(blk):
        for cp in copies(lambda a: outs[a].at[blk], blk, far_s, 0, to_far):
            cp.wait_recv()

    def sent(sem, slot, dev):
        for cp in copies(lambda a: ins[a], 0, sem, slot, dev):
            cp.wait_send()

    own = lambda a: ins[a]
    me = ep * sub_size + sub
    pl.when(sub < last)(lambda: start(own, me, right_s, sub, to_right))
    pl.when(sub > 0)(lambda: start(own, me, left_s, sub, to_left))
    start(own, me, far_s, sub, to_far)
    start(own, me, core_s, sub, to_core)
    for a in range(count):
        cp = pltpu.make_async_copy(ins[a], stage[a], loc.at[a])
        cp.start()
        cp.wait()
    for a in range(count):
        pltpu.make_async_copy(stage[a], outs[a].at[me], loc.at[a]).start()

    def from_far(src_sub):
        blk = ep_far * sub_size + src_sub
        landed(blk)
        start(lambda a: outs[a].at[blk], blk, core_s, sub_size + src_sub, to_core)

    def from_line(src_sub, sem, cond, dev):
        blk = ep * sub_size + src_sub
        src = lambda a: outs[a].at[blk]
        landed(blk)
        pl.when(cond)(lambda: start(src, blk, sem, src_sub, dev))
        start(src, blk, far_s, src_sub, to_far)
        start(src, blk, core_s, src_sub, to_core)

    for dist in range(1, sub_size):
        pl.when(sub - dist >= 0)(lambda: from_line(sub - dist, right_s, sub < last, to_right))
        pl.when(sub + dist <= last)(lambda: from_line(sub + dist, left_s, sub > 0, to_left))
        if dist == 1:
            from_far(sub)
        else:
            pl.when(sub - dist + 1 >= 0)(lambda: from_far(sub - dist + 1))
            pl.when(sub + dist - 1 <= last)(lambda: from_far(sub + dist - 1))
    pl.when(sub - last >= 0)(lambda: from_far(sub - last))
    pl.when(sub + last <= last)(lambda: from_far(sub + last))

    for src_sub in range(sub_size):
        landed(ep_core * sub_size + src_sub)
        landed(ep_diag * sub_size + src_sub)
    for src_sub in range(sub_size):
        sent(far_s, src_sub, to_far)
        sent(core_s, src_sub, to_core)
        sent(core_s, sub_size + src_sub, to_core)
        pl.when((sub >= src_sub) & (sub < last))(lambda: sent(right_s, src_sub, to_right))
        pl.when((sub <= src_sub) & (sub > 0))(lambda: sent(left_s, src_sub, to_left))
    for a in range(count):
        pltpu.make_async_copy(stage[a], outs[a].at[me], loc.at[a]).wait()


def gather_tokens(arrays, num_dev, sub_size, collective_id):
    count = len(arrays)
    sems = lambda n: pltpu.SemaphoreType.DMA((count, n))
    return pl.pallas_call(
        functools.partial(gather_body, count, sub_size),
        out_shape=[jax.ShapeDtypeStruct((num_dev,) + a.shape, a.dtype) for a in arrays],
        in_specs=[pl.BlockSpec(memory_space=pl.ANY)] * count,
        out_specs=[pl.BlockSpec(memory_space=pl.ANY)] * count,
        scratch_shapes=[pltpu.VMEM(a.shape, a.dtype) for a in arrays] + [sems(num_dev), sems(sub_size), sems(sub_size), sems(sub_size), sems(2 * sub_size), pltpu.SemaphoreType.DMA((count,))],
        compiler_params=pltpu.CompilerParams(collective_id=collective_id, has_side_effects=True, vmem_limit_bytes=VMEM_CAP),
        name='gather_tokens',
    )(*arrays)


def pick_body(exp_local, cap_slots, base_ref, code_ref, tok_ref, out_ref):
    room = exp_local * cap_slots
    top_k, tok_count = code_ref.shape[1] // 2, code_ref.shape[2]
    want = lax.broadcasted_iota(jnp.int32, (room, tok_count), 0).astype(jnp.float32) + base_ref[0].astype(jnp.float32)
    hit = code_ref[0, 0:1, :] == want
    for j in range(1, top_k):
        hit = hit | (code_ref[0, j:j + 1, :] == want)
    onehot = jnp.where(hit, 1.0, 0.0).astype(jnp.bfloat16)
    picked = jnp.dot(onehot, tok_ref[0], preferred_element_type=jnp.float32).astype(jnp.bfloat16)
    for e in range(exp_local):
        out_ref[e] = picked[e * cap_slots:(e + 1) * cap_slots]


def pick_rows(base, codes, gathered, exp_local, cap_slots):
    num_dev, tok_count, dim = gathered.shape
    return pl.pallas_call(
        functools.partial(pick_body, exp_local, cap_slots),
        grid=(num_dev,),
        out_shape=jax.ShapeDtypeStruct((exp_local, num_dev * cap_slots, dim), jnp.bfloat16),
        in_specs=[
            pl.BlockSpec(memory_space=pltpu.SMEM),
            pl.BlockSpec((1,) + codes.shape[1:], lambda s: (s, 0, 0)),
            pl.BlockSpec((1, tok_count, dim), lambda s: (s, 0, 0)),
        ],
        out_specs=pl.BlockSpec((exp_local, cap_slots, dim), lambda s: (0, s, 0)),
        compiler_params=pltpu.CompilerParams(vmem_limit_bytes=VMEM_CAP),
        name='pick_rows',
    )(base, codes, gathered)


def ffn_body(steps, x_ref, w1_ref, w3_ref, w2_ref, out_ref, act_ref):
    step = pl.program_id(1)

    @pl.when(step < steps)
    def _():
        x = x_ref[0]
        gate_h = jnp.dot(x, w1_ref[0], preferred_element_type=jnp.float32)
        up_h = jnp.dot(x, w3_ref[0], preferred_element_type=jnp.float32)
        act_ref[step] = (jax.nn.silu(gate_h) * up_h).astype(jnp.bfloat16)

    @pl.when(step >= steps)
    def _():
        tile = w2_ref.shape[1] // steps
        acc = jnp.dot(act_ref[0], w2_ref[0, 0:tile, :], preferred_element_type=jnp.float32)
        for k in range(1, steps):
            acc = acc + jnp.dot(act_ref[k], w2_ref[0, k * tile:(k + 1) * tile, :], preferred_element_type=jnp.float32)
        out_ref[...] = acc.astype(jnp.bfloat16).reshape(out_ref.shape)


def expert_ffn(rows, w_gate, w_up, w_down, num_dev, cap_slots):
    exp_local, room, dim = rows.shape
    ff = w_gate.shape[2]
    steps = 4
    ft, nt = ff // steps, dim // steps
    return pl.pallas_call(
        functools.partial(ffn_body, steps),
        grid=(exp_local, 2 * steps),
        out_shape=jax.ShapeDtypeStruct((num_dev, exp_local, cap_slots, dim), jnp.bfloat16),
        in_specs=[
            pl.BlockSpec((1, room, dim), lambda e, s: (e, 0, 0)),
            pl.BlockSpec((1, dim, ft), lambda e, s: (e, 0, jnp.minimum(s, steps - 1))),
            pl.BlockSpec((1, dim, ft), lambda e, s: (e, 0, jnp.minimum(s, steps - 1))),
            pl.BlockSpec((1, ff, nt), lambda e, s: (e, 0, jnp.maximum(s - steps, 0))),
        ],
        out_specs=pl.BlockSpec((num_dev, 1, cap_slots, nt), lambda e, s: (0, e, 0, jnp.maximum(s - steps, 0))),
        scratch_shapes=[pltpu.VMEM((steps, room, ft), jnp.bfloat16)],
        compiler_params=pltpu.CompilerParams(vmem_limit_bytes=VMEM_CAP),
        name='expert_ffn',
    )(rows, w_gate, w_up, w_down)


PARTS = 2


def combine_body(sub_size, e_ref, col_ref, gate_ref, hid_ref, out_ref, slots, sums, from_left, from_right, mix, a_recv, a_send, a_loc, l_recv, r_recv, z_send):
    ep, sub = lax.axis_index('ep'), lax.axis_index('sub')
    ep_far = lax.rem(ep + 2, 4)
    ep_core = ep + 1 - 2 * lax.rem(ep, 2)
    ep_diag = lax.rem(ep_core + 2, 4)
    last = sub_size - 1
    room, dim = e_ref.shape[1], e_ref.shape[2]
    tok_count, top_k = col_ref.shape[1], col_ref.shape[2]
    width = dim // PARTS
    to_right, to_left = {'ep': ep, 'sub': sub + 1}, {'ep': ep, 'sub': sub - 1}
    peers = [ep_far, ep_diag, ep_core]
    greet(sub, sub_size, [{'ep': p, 'sub': sub} for p in peers], to_left, to_right)

    side = sub // 2
    near = sub + side * (3 - 2 * sub)
    order = [a + side * (3 - 2 * a) for a in (3, 2 - 2 * near, 1 + near, near)]

    def part(h):
        return pl.ds(h * width, width)

    def slot_copy(dst, k, h):
        peer = peers[k]
        return pltpu.make_async_remote_copy(
            src_ref=e_ref.at[peer * sub_size + dst, :, part(h)], dst_ref=slots.at[dst, pl.ds(pl.multiple_of(ep * room, room), room), part(h)],
            send_sem=a_send.at[dst, k, h], recv_sem=a_recv.at[dst, ep, h], device_id={'ep': peer, 'sub': sub}, device_id_type=MESH)

    def slot_landed(dst, k, h):
        peer = peers[k]
        pltpu.make_async_remote_copy(
            src_ref=e_ref.at[peer * sub_size + dst, :, part(h)], dst_ref=slots.at[dst, pl.ds(pl.multiple_of(peer * room, room), room), part(h)],
            send_sem=a_send.at[dst, k, h], recv_sem=a_recv.at[dst, peer, h], device_id={'ep': peer, 'sub': sub}, device_id_type=MESH).wait_recv()

    def own_copy(dst):
        return pltpu.make_async_copy(e_ref.at[ep * sub_size + dst], slots.at[dst, pl.ds(pl.multiple_of(ep * room, room), room), :], a_loc.at[dst])

    def line_copy(dst, h, right):
        inbox, sem, dev = (from_left, l_recv, to_right) if right else (from_right, r_recv, to_left)
        return pltpu.make_async_remote_copy(
            src_ref=sums.at[dst, :, part(h)], dst_ref=inbox.at[dst, :, part(h)],
            send_sem=z_send.at[dst, h], recv_sem=sem.at[dst, h], device_id=dev, device_id_type=MESH)

    for dst in order:
        for h in range(PARTS):
            for k in range(3):
                slot_copy(dst, k, h).start()
        own_copy(dst).start()

    for i, dst in enumerate(order):
        cols = lax.broadcasted_iota(jnp.int32, (tok_count, 4 * room), 1)
        mat = jnp.zeros((tok_count, 4 * room), jnp.float32)
        for j in range(top_k):
            mat = jnp.where(col_ref[dst, :, j:j + 1] == cols, gate_ref[dst, :, j:j + 1], mat)
        for s in range(3):
            piece = mat.astype(jnp.bfloat16)
            mix[s * tok_count:(s + 1) * tok_count, :] = piece
            mat = mat - piece.astype(jnp.float32)
        own_copy(dst).wait()
        for h in range(PARTS):
            for k in range(3):
                slot_landed(dst, k, h)
            tile = 256
            for c in range(width // tile):
                cs = pl.ds(h * width + c * tile, tile)
                prod = jnp.dot(mix[...], slots[dst, :, cs], preferred_element_type=jnp.float32)
                sums[dst, :, cs] = prod[0:tok_count] + (prod[tok_count:2 * tok_count] + prod[2 * tok_count:])

            def add(inbox, sem, right):
                line_copy(dst, h, right).wait_recv()
                sums[dst, :, part(h)] = sums[dst, :, part(h)] + inbox[dst, :, part(h)]

            if i < last:
                pl.when((dst > sub) & (sub > 0))(lambda: add(from_left, l_recv, True))
                pl.when((dst < sub) & (sub < last))(lambda: add(from_right, r_recv, False))
                pl.when(dst > sub)(lambda: line_copy(dst, h, True).start())
                pl.when(dst < sub)(lambda: line_copy(dst, h, False).start())
            else:
                pl.when(sub > 0)(lambda: add(from_left, l_recv, True))
                pl.when(sub < last)(lambda: add(from_right, r_recv, False))
                out_ref[:, part(h)] = (hid_ref[:, part(h)].astype(jnp.float32) + sums[dst, :, part(h)]).astype(jnp.bfloat16)

    for i, dst in enumerate(order):
        for h in range(PARTS):
            for k in range(3):
                slot_copy(dst, k, h).wait_send()
            if i < last:
                pl.when(dst > sub)(lambda: line_copy(dst, h, True).wait_send())
                pl.when(dst < sub)(lambda: line_copy(dst, h, False).wait_send())


def combine_rows(expert_rows, cols, gates, hidden, sub_size, collective_id):
    num_dev, room, dim = expert_rows.shape
    tok_count = hidden.shape[0]
    dma = lambda *s: pltpu.SemaphoreType.DMA(s)
    vmem = pl.BlockSpec(memory_space=pltpu.VMEM)
    return pl.pallas_call(
        functools.partial(combine_body, sub_size),
        out_shape=jax.ShapeDtypeStruct((tok_count, dim), jnp.bfloat16),
        in_specs=[pl.BlockSpec(memory_space=pl.ANY), vmem, vmem, vmem],
        out_specs=vmem,
        scratch_shapes=[
            pltpu.VMEM((sub_size, 4 * room, dim), jnp.bfloat16),
            pltpu.VMEM((sub_size, tok_count, dim), jnp.float32),
            pltpu.VMEM((sub_size, tok_count, dim), jnp.float32),
            pltpu.VMEM((sub_size, tok_count, dim), jnp.float32),
            pltpu.VMEM((3 * tok_count, 4 * room), jnp.bfloat16),
            dma(sub_size, 4, PARTS), dma(sub_size, 3, PARTS), dma(sub_size,),
            dma(sub_size, PARTS), dma(sub_size, PARTS), dma(sub_size, PARTS),
        ],
        compiler_params=pltpu.CompilerParams(collective_id=collective_id, has_side_effects=True, vmem_limit_bytes=VMEM_CAP),
        name='combine_rows',
    )(expert_rows, cols, gates, hidden)


def solution(mesh):
    ep_size = mesh.shape['ep']
    sub_size = mesh.shape['sub']
    num_dev = ep_size * sub_size
    tok_spec = P(('dp', 'ep', 'sub'), None, None)
    route_spec = P(None, ('dp', 'ep', 'sub'), None)
    exp_spec = P(('ep', 'sub'), None, None)

    def device_body(input_a, input_b, route_idx, route_gate, attn_norm, w_query, w_key, w_value, w_out, moe_norm, w_gate, w_up, w_down):
        exp_local = w_gate.shape[0]
        num_exp = exp_local * num_dev
        tok_count, top_k = route_idx.shape[1:]
        dim = input_a.shape[2]
        cap_slots = 3 * top_k * tok_count // (2 * num_exp)
        room = exp_local * cap_slots
        ep, sub = lax.axis_index('ep'), lax.axis_index('sub')

        meta = jnp.concatenate([jnp.stack([slot_codes(route_idx[m], num_exp, cap_slots) for m in range(2)]), route_gate], axis=2)
        meta = meta.transpose(0, 2, 1)
        hidden = [attention_block(x, attn_norm, w_query, w_key, w_value, w_out).reshape(tok_count, dim) for x in (input_a, input_b)]
        normed = [rms_norm(h, moe_norm) for h in hidden]
        gath_a, metas = gather_tokens([normed[0], meta], num_dev, sub_size, 1)
        gath_b, = gather_tokens([normed[1]], num_dev, sub_size, 2)
        base = ((ep * sub_size + sub) * room).astype(jnp.int32).reshape(1)
        mine = lax.dynamic_slice_in_dim(metas, ep * sub_size, sub_size, axis=0)
        code = mine[:, :, :top_k, :].astype(jnp.int32).transpose(1, 0, 3, 2)
        gates = mine[:, :, top_k:, :].transpose(1, 0, 3, 2)
        dev_of = code // room
        cols = jnp.where(dev_of % sub_size == sub, (dev_of // sub_size) * room + code % room, -1)
        outs = []
        for m, gathered in enumerate((gath_a, gath_b)):
            rows = pick_rows(base, metas[:, m], gathered, exp_local, cap_slots)
            expert_rows = expert_ffn(rows, w_gate, w_up, w_down, num_dev, cap_slots).reshape(num_dev, room, dim)
            outs.append(combine_rows(expert_rows, cols[m], gates[m], hidden[m], sub_size, 3 + m).reshape(1, tok_count, dim))
        return tuple(outs)

    return jax.shard_map(device_body, mesh=mesh, in_specs=(tok_spec, tok_spec, route_spec, route_spec, P(), P(), P(), P(), P(), P(), exp_spec, exp_spec, exp_spec), out_specs=(tok_spec, tok_spec), check_vma=False)
```

```python
import functools

import jax
import jax.numpy as jnp
from jax import lax
from jax.experimental import pallas as pl
from jax.experimental.pallas import tpu as pltpu
from jax.sharding import PartitionSpec as P

NORM_EPS = 1e-6
MESH = pl.DeviceIdType.MESH
VMEM_CAP = 60 * 1024 * 1024
ANY = pl.BlockSpec(memory_space=pl.ANY)


def rms_norm(values, norm_gain):
    acc_f32 = values.astype(jnp.float32)
    inv_rms = lax.rsqrt(jnp.mean(acc_f32 * acc_f32, axis=-1, keepdims=True) + NORM_EPS)
    return (acc_f32 * inv_rms * norm_gain).astype(jnp.bfloat16)


def attention_block(tokens, attn_norm, w_query, w_key, w_value, w_out):
    normed = rms_norm(tokens, attn_norm)
    q_heads = jnp.einsum('bsd,dhc->bshc', normed, w_query, preferred_element_type=jnp.float32).astype(jnp.bfloat16)
    k_heads = jnp.einsum('bsd,dhc->bshc', normed, w_key, preferred_element_type=jnp.float32).astype(jnp.bfloat16)
    v_heads = jnp.einsum('bsd,dhc->bshc', normed, w_value, preferred_element_type=jnp.float32).astype(jnp.bfloat16)
    score_scale = w_query.shape[2] ** -0.5
    scores = jnp.einsum('bqhc,bkhc->bhqk', q_heads, k_heads, preferred_element_type=jnp.float32) * score_scale
    seq_len = tokens.shape[1]
    causal = lax.broadcasted_iota(jnp.int32, (seq_len, seq_len), 0) >= lax.broadcasted_iota(jnp.int32, (seq_len, seq_len), 1)
    scores = jnp.where(causal, scores, -jnp.inf)
    prob_bf = jax.nn.softmax(scores, axis=-1).astype(jnp.bfloat16)
    context = jnp.einsum('bhqk,bkhc->bqhc', prob_bf, v_heads, preferred_element_type=jnp.float32).astype(jnp.bfloat16)
    proj_out = jnp.einsum('crid,ide->cre', context, w_out, preferred_element_type=jnp.float32)
    return (tokens.astype(jnp.float32) + proj_out).astype(jnp.bfloat16)


def slot_codes(exp_ids, num_exp, cap_slots):
    hits = exp_ids[:, :, None] == jnp.arange(num_exp, dtype=jnp.int32)[None, None, :]
    chosen = jnp.any(hits, axis=1)
    tok_count = exp_ids.shape[0]
    before = lax.broadcasted_iota(jnp.int32, (tok_count, tok_count), 0) > lax.broadcasted_iota(jnp.int32, (tok_count, tok_count), 1)
    rank = jnp.dot(before.astype(jnp.bfloat16), chosen.astype(jnp.bfloat16), preferred_element_type=jnp.float32)
    rank_of = jnp.sum(jnp.where(hits, rank[:, None, :], 0.0), axis=2)
    return exp_ids.astype(jnp.float32) * cap_slots + rank_of


def greet(sub, sub_size, peers, to_left, to_right):
    barrier = pltpu.get_barrier_semaphore()
    last = sub_size - 1

    def hello(dev):
        pl.semaphore_signal(barrier, inc=1, device_id=dev, device_id_type=MESH)

    for dev in peers:
        hello(dev)
    pl.when(sub > 0)(lambda: hello(to_left))
    pl.when(sub < last)(lambda: hello(to_right))
    pl.semaphore_wait(barrier, len(peers) + (sub + last) // sub_size + (2 * last - sub) // sub_size)


class Gather:
    def __init__(self, sub_size, ins, outs, stage, recv, right_s, left_s, far_s, core_s, loc):
        self.count, self.sub_size = len(ins), sub_size
        self.ins, self.outs, self.stage = ins, outs, stage
        self.recv, self.right_s, self.left_s, self.far_s, self.core_s, self.loc = recv, right_s, left_s, far_s, core_s, loc
        ep, sub = lax.axis_index('ep'), lax.axis_index('sub')
        self.ep, self.sub, self.last = ep, sub, sub_size - 1
        self.ep_far = lax.rem(ep + 2, 4)
        self.ep_core = ep + 1 - 2 * lax.rem(ep, 2)
        self.ep_diag = lax.rem(self.ep_core + 2, 4)
        self.me = ep * sub_size + sub
        self.to_right, self.to_left = {'ep': ep, 'sub': sub + 1}, {'ep': ep, 'sub': sub - 1}
        self.to_far, self.to_core = {'ep': self.ep_far, 'sub': sub}, {'ep': self.ep_core, 'sub': sub}

    def copies(self, src, blk, sem, slot, dev):
        return [pltpu.make_async_remote_copy(src_ref=src(a), dst_ref=self.outs[a].at[blk], send_sem=sem.at[a, slot], recv_sem=self.recv.at[a, blk], device_id=dev, device_id_type=MESH) for a in range(self.count)]

    def start(self, *args):
        for cp in self.copies(*args):
            cp.start()

    def landed(self, blk):
        for cp in self.copies(lambda a: self.outs[a].at[blk], blk, self.far_s, 0, self.to_far):
            cp.wait_recv()

    def sent(self, sem, slot, dev):
        for cp in self.copies(lambda a: self.ins[a], 0, sem, slot, dev):
            cp.wait_send()

    def begin(self):
        own = lambda a: self.ins[a]
        sub, me = self.sub, self.me
        greet(sub, self.sub_size, [self.to_far, self.to_core], self.to_left, self.to_right)
        pl.when(sub < self.last)(lambda: self.start(own, me, self.right_s, sub, self.to_right))
        pl.when(sub > 0)(lambda: self.start(own, me, self.left_s, sub, self.to_left))
        self.start(own, me, self.far_s, sub, self.to_far)
        self.start(own, me, self.core_s, sub, self.to_core)
        for a in range(self.count):
            cp = pltpu.make_async_copy(self.ins[a], self.stage[a], self.loc.at[a])
            cp.start()
            cp.wait()
        for a in range(self.count):
            pltpu.make_async_copy(self.stage[a], self.outs[a].at[me], self.loc.at[a]).start()

    def from_far(self, src_sub):
        blk = self.ep_far * self.sub_size + src_sub
        self.landed(blk)
        self.start(lambda a: self.outs[a].at[blk], blk, self.core_s, self.sub_size + src_sub, self.to_core)

    def from_line(self, src_sub, sem, cond, dev):
        blk = self.ep * self.sub_size + src_sub
        src = lambda a: self.outs[a].at[blk]
        self.landed(blk)
        pl.when(cond)(lambda: self.start(src, blk, sem, src_sub, dev))
        self.start(src, blk, self.far_s, src_sub, self.to_far)
        self.start(src, blk, self.core_s, src_sub, self.to_core)

    def hop(self, dist):
        sub, last = self.sub, self.last
        pl.when(sub - dist >= 0)(lambda: self.from_line(sub - dist, self.right_s, sub < last, self.to_right))
        pl.when(sub + dist <= last)(lambda: self.from_line(sub + dist, self.left_s, sub > 0, self.to_left))
        if dist == 1:
            self.from_far(sub)
        else:
            pl.when(sub - dist + 1 >= 0)(lambda: self.from_far(sub - dist + 1))
            pl.when(sub + dist - 1 <= last)(lambda: self.from_far(sub + dist - 1))

    def end(self):
        sub, last, size = self.sub, self.last, self.sub_size
        pl.when(sub - last >= 0)(lambda: self.from_far(sub - last))
        pl.when(sub + last <= last)(lambda: self.from_far(sub + last))
        for src_sub in range(size):
            self.landed(self.ep_core * size + src_sub)
            self.landed(self.ep_diag * size + src_sub)
        for src_sub in range(size):
            self.sent(self.far_s, src_sub, self.to_far)
            self.sent(self.core_s, src_sub, self.to_core)
            self.sent(self.core_s, size + src_sub, self.to_core)
            pl.when((sub >= src_sub) & (sub < last))(lambda: self.sent(self.right_s, src_sub, self.to_right))
            pl.when((sub <= src_sub) & (sub > 0))(lambda: self.sent(self.left_s, src_sub, self.to_left))
        for a in range(self.count):
            pltpu.make_async_copy(self.stage[a], self.outs[a].at[self.me], self.loc.at[a]).wait()


def gather_scratch(arrays, num_dev, sub_size):
    sems = lambda n: pltpu.SemaphoreType.DMA((len(arrays), n))
    return [pltpu.VMEM(a.shape, a.dtype) for a in arrays] + [sems(num_dev), sems(sub_size), sems(sub_size), sems(sub_size), sems(2 * sub_size), pltpu.SemaphoreType.DMA((len(arrays),))]


def gather_body(count, sub_size, *refs):
    g = Gather(sub_size, refs[:count], refs[count:2 * count], refs[2 * count:3 * count], *refs[3 * count:])
    g.begin()
    for dist in range(1, sub_size):
        g.hop(dist)
    g.end()


def gather_tokens(arrays, num_dev, sub_size, collective_id):
    count = len(arrays)
    return pl.pallas_call(
        functools.partial(gather_body, count, sub_size),
        out_shape=[jax.ShapeDtypeStruct((num_dev,) + a.shape, a.dtype) for a in arrays],
        in_specs=[ANY] * count,
        out_specs=[ANY] * count,
        scratch_shapes=gather_scratch(arrays, num_dev, sub_size),
        compiler_params=pltpu.CompilerParams(collective_id=collective_id, has_side_effects=True, vmem_limit_bytes=VMEM_CAP),
        name='gather_tokens',
    )(*arrays)


FFN_STEPS = 4


def run_experts(mb, me, gath, metas, w1, w3, w2, rows, e_out, act_ref, after_pick, hook):
    num_dev, exp_local, cap_slots, dim = e_out.shape
    tok_count = gath.shape[1]
    top_k = metas.shape[2] // 2
    ff = w1.shape[2]
    room = exp_local * cap_slots
    steps = FFN_STEPS
    ft, nt = ff // steps, dim // steps
    base = (me * room).astype(jnp.float32)

    def pick(code_ref, tok_ref, out_ref):
        want = lax.broadcasted_iota(jnp.int32, (room, tok_count), 0).astype(jnp.float32) + base
        hit = code_ref[0, 0, 0:1, :] == want
        for j in range(1, top_k):
            hit = hit | (code_ref[0, 0, j:j + 1, :] == want)
        onehot = jnp.where(hit, 1.0, 0.0).astype(jnp.bfloat16)
        picked = jnp.dot(onehot, tok_ref[0], preferred_element_type=jnp.float32).astype(jnp.bfloat16)
        for e in range(exp_local):
            out_ref[e] = picked[e * cap_slots:(e + 1) * cap_slots]

    pltpu.emit_pipeline(
        pick,
        grid=(num_dev,),
        in_specs=[pl.BlockSpec((1, 1) + metas.shape[2:], lambda s: (s, mb, 0, 0)), pl.BlockSpec((1, tok_count, dim), lambda s: (s, 0, 0))],
        out_specs=[pl.BlockSpec((exp_local, cap_slots, dim), lambda s: (0, s, 0))],
    )(metas, gath, rows)
    after_pick()

    def ffn(indices, x_ref, w1_ref, w3_ref, w2_ref, out_ref):
        e, step = indices.index

        @pl.when(step < steps)
        def _():
            x = x_ref[0]
            gate_h = jnp.dot(x, w1_ref[0], preferred_element_type=jnp.float32)
            up_h = jnp.dot(x, w3_ref[0], preferred_element_type=jnp.float32)
            act_ref[step] = (jax.nn.silu(gate_h) * up_h).astype(jnp.bfloat16)

        @pl.when(step >= steps)
        def _():
            acc = jnp.dot(act_ref[0], w2_ref[0, 0:ft, :], preferred_element_type=jnp.float32)
            for k in range(1, steps):
                acc = acc + jnp.dot(act_ref[k], w2_ref[0, k * ft:(k + 1) * ft, :], preferred_element_type=jnp.float32)
            out_ref[...] = acc.astype(jnp.bfloat16).reshape(out_ref.shape)

        hook(e, step)

    pltpu.emit_pipeline(
        ffn,
        grid=(exp_local, 2 * steps),
        in_specs=[
            pl.BlockSpec((1, num_dev * cap_slots, dim), lambda e, s: (e, 0, 0)),
            pl.BlockSpec((1, dim, ft), lambda e, s: (e, 0, jnp.minimum(s, steps - 1))),
            pl.BlockSpec((1, dim, ft), lambda e, s: (e, 0, jnp.minimum(s, steps - 1))),
            pl.BlockSpec((1, ff, nt), lambda e, s: (e, 0, jnp.maximum(s - steps, 0))),
        ],
        out_specs=[pl.BlockSpec((num_dev, 1, cap_slots, nt), lambda e, s: (0, e, 0, jnp.maximum(s - steps, 0)))],
        _explicit_indices=True,
    )(rows, w1, w3, w2, e_out)


def expert_shapes(num_dev, exp_local, cap_slots, dim):
    return [jax.ShapeDtypeStruct((exp_local, num_dev * cap_slots, dim), jnp.bfloat16), jax.ShapeDtypeStruct((num_dev, exp_local, cap_slots, dim), jnp.bfloat16)]


def act_scratch(num_dev, cap_slots, ff):
    return pltpu.VMEM((FFN_STEPS, num_dev * cap_slots, ff // FFN_STEPS), jnp.bfloat16)


def first_body(sub_size, norm_b, gath_a, metas, w1, w3, w2, gath_b, rows, e_a, act_ref, stage, *sems):
    g = Gather(sub_size, [norm_b], [gath_b], [stage], *sems)
    g.begin()

    def hook(e, step):
        pl.when((e == 1) & (step == 4))(lambda: g.hop(2))
        pl.when((e == 3) & (step == 1))(lambda: g.hop(3))

    run_experts(0, g.me, gath_a, metas, w1, w3, w2, rows, e_a, act_ref, lambda: g.hop(1), hook)
    g.end()


def first_experts(norm_b, gath_a, metas, w1, w3, w2, cap_slots, sub_size, collective_id):
    num_dev, tok_count, dim = gath_a.shape
    exp_local, _, ff = w1.shape
    return pl.pallas_call(
        functools.partial(first_body, sub_size),
        out_shape=[jax.ShapeDtypeStruct(gath_a.shape, gath_a.dtype)] + expert_shapes(num_dev, exp_local, cap_slots, dim),
        in_specs=[ANY] * 6,
        out_specs=[ANY] * 3,
        scratch_shapes=[act_scratch(num_dev, cap_slots, ff)] + gather_scratch([norm_b], num_dev, sub_size),
        compiler_params=pltpu.CompilerParams(collective_id=collective_id, has_side_effects=True, vmem_limit_bytes=VMEM_CAP),
        name='first_experts',
    )(norm_b, gath_a, metas, w1, w3, w2)


PARTS = 2


class Combine:
    def __init__(self, mb, sub_size, e_ref, metas, hid, out, land, inbox, sums, mix, tile, a_recv, a_send, z_recv, z_send, loads):
        self.mb, self.sub_size, self.last = mb, sub_size, sub_size - 1
        self.e_ref, self.metas, self.hid, self.out, self.land = e_ref, metas, hid, out, land
        self.inbox, self.sums, self.mix, self.tile = inbox, sums, mix, tile
        self.a_recv, self.a_send, self.z_recv, self.z_send, self.loads = a_recv, a_send, z_recv, z_send, loads
        ep, sub = lax.axis_index('ep'), lax.axis_index('sub')
        self.ep, self.sub = ep, sub
        ep_far = lax.rem(ep + 2, 4)
        ep_core = ep + 1 - 2 * lax.rem(ep, 2)
        self.peers = [ep_far, lax.rem(ep_core + 2, 4), ep_core]
        self.to_right, self.to_left = {'ep': ep, 'sub': sub + 1}, {'ep': ep, 'sub': sub - 1}
        self.width = e_ref.shape[3] // PARTS

    def greet(self):
        greet(self.sub, self.sub_size, [{'ep': p, 'sub': self.sub} for p in self.peers], self.to_left, self.to_right)

    def order(self, i):
        side = self.sub // 2
        near = self.sub + side * (3 - 2 * self.sub)
        a = 3 - i + near * (3 * (i // 2) - 2 * ((i + 2) // 3))
        return a + side * (3 - 2 * a)

    def part(self, h):
        return pl.ds(pl.multiple_of(h * self.width, self.width), self.width)

    def slot_copy(self, dst, k, h, src_ep):
        return pltpu.make_async_remote_copy(
            src_ref=self.e_ref.at[self.peers[k] * self.sub_size + dst, :, :, self.part(h)], dst_ref=self.land.at[dst, src_ep, :, :, self.part(h)],
            send_sem=self.a_send.at[self.mb, dst, k, h], recv_sem=self.a_recv.at[self.mb, dst, src_ep, h], device_id={'ep': self.peers[k], 'sub': self.sub}, device_id_type=MESH)

    def line_copy(self, dst, h, box, dev):
        return pltpu.make_async_remote_copy(
            src_ref=self.sums.at[dst, :, self.part(h)], dst_ref=self.inbox.at[self.mb, box, :, self.part(h)],
            send_sem=self.z_send.at[self.mb, dst, h], recv_sem=self.z_recv.at[self.mb, box, h], device_id=dev, device_id_type=MESH)

    def begin(self):
        @pl.loop(0, self.sub_size * PARTS)
        def _(t):
            dst = self.order(t // PARTS)
            for k in range(3):
                self.slot_copy(dst, k, t % PARTS, self.ep).start()

    def build_mix(self, dst):
        tok_count, room = self.sums.shape[1], self.e_ref.shape[1] * self.e_ref.shape[2]
        cols = lax.broadcasted_iota(jnp.int32, (tok_count, 4 * room), 1)
        want = (cols + (cols // room) * ((self.sub_size - 1) * room) + self.sub * room).astype(jnp.float32)
        route = self.metas[self.ep * self.sub_size + dst, self.mb].T
        top_k = route.shape[1] // 2
        mat = jnp.zeros((tok_count, 4 * room), jnp.float32)
        for j in range(top_k):
            mat = jnp.where(route[:, j:j + 1] == want, route[:, top_k + j:top_k + j + 1], mat)
        for s in range(3):
            piece = mat.astype(jnp.bfloat16)
            self.mix[s * tok_count:(s + 1) * tok_count, :] = piece
            mat = mat - piece.astype(jnp.float32)

    def event(self, t):
        i, h = t // PARTS, t % PARTS
        dst, sub, last = self.order(i), self.sub, self.last
        tok_count = self.sums.shape[1]
        pl.when(h == 0)(lambda: self.build_mix(dst))
        for k in range(3):
            self.slot_copy(dst, k, h, self.peers[k]).wait_recv()
        pulls = [pltpu.make_async_copy(self.land.at[dst, p, :, :, self.part(h)], self.tile.at[p], self.loads.at[p]) for p in self.peers]
        pulls.append(pltpu.make_async_copy(self.e_ref.at[self.ep * self.sub_size + dst, :, :, self.part(h)], self.tile.at[self.ep], self.loads.at[self.ep]))
        for cp in pulls:
            cp.start()
        for cp in pulls:
            cp.wait()
        cut = 256

        @pl.loop(0, self.width // cut)
        def _(c):
            rows = self.tile[:, :, :, pl.ds(pl.multiple_of(c * cut, cut), cut)].reshape(self.mix.shape[1], cut)
            prod = jnp.dot(self.mix[...], rows, preferred_element_type=jnp.float32)
            self.sums[dst, :, pl.ds(pl.multiple_of(h * self.width + c * cut, cut), cut)] = prod[0:tok_count] + (prod[tok_count:2 * tok_count] + prod[2 * tok_count:])

        def add(box):
            self.line_copy(dst, h, box, self.to_left).wait_recv()
            self.sums[dst, :, self.part(h)] = self.sums[dst, :, self.part(h)] + self.inbox[self.mb, box, :, self.part(h)]

        size = self.sub_size
        pl.when((dst >= sub) & (sub > 0))(lambda: add(dst))
        pl.when((dst <= sub) & (sub < last))(lambda: add(dst + (1 - (sub - dst + last) // size) * (size - dst)))
        pl.when(dst > sub)(lambda: self.line_copy(dst, h, dst, self.to_right).start())
        pl.when(dst < sub)(lambda: self.line_copy(dst, h, dst + (1 - (sub - 1 - dst + last) // size) * (size - dst), self.to_left).start())

        @pl.when(dst == sub)
        def _():
            self.out[:, self.part(h)] = (self.hid[:, self.part(h)].astype(jnp.float32) + self.sums[dst, :, self.part(h)]).astype(jnp.bfloat16)

    def end(self):
        @pl.loop(0, self.sub_size * PARTS)
        def _(t):
            h = t % PARTS
            dst = self.order(t // PARTS)
            for k in range(3):
                self.slot_copy(dst, k, h, self.ep).wait_send()
            pl.when(dst != self.sub)(lambda: self.line_copy(dst, h, dst, self.to_right).wait_send())


def second_body(sub_size, e_a, gath_b, metas_any, w1, w3, w2, metas, hid_a, hid_b, out_a, out_b, land_a, land_b, rows, e_b, act_ref, inbox, sums, mix, tile, *sems):
    com_a = Combine(0, sub_size, e_a, metas, hid_a, out_a, land_a, inbox, sums, mix, tile, *sems)
    com_b = Combine(1, sub_size, e_b, metas, hid_b, out_b, land_b, inbox, sums, mix, tile, *sems)
    com_a.greet()
    com_a.begin()
    me = com_a.ep * sub_size + com_a.sub
    events = sub_size * PARTS

    def hook(e, step):
        pl.when(step == 2 * FFN_STEPS - 1)(lambda: com_a.event(e + 1))

    run_experts(1, me, gath_b, metas_any, w1, w3, w2, rows, e_b, act_ref, lambda: com_a.event(0), hook)
    com_b.begin()
    pl.loop(w1.shape[0] + 1, events)(com_a.event)
    com_a.end()
    pl.loop(0, events)(com_b.event)
    com_b.end()


def second_experts(e_a, gath_b, metas, w1, w3, w2, hid_a, hid_b, sub_size, collective_id):
    num_dev, exp_local, cap_slots, dim = e_a.shape
    tok_count = hid_a.shape[0]
    ff = w1.shape[2]
    room = exp_local * cap_slots
    dma = lambda *s: pltpu.SemaphoreType.DMA(s)
    land = jax.ShapeDtypeStruct((sub_size, 4, exp_local, cap_slots, dim), jnp.bfloat16)
    hid = jax.ShapeDtypeStruct((tok_count, dim), jnp.bfloat16)
    vmem = pl.BlockSpec(memory_space=pltpu.VMEM)
    return pl.pallas_call(
        functools.partial(second_body, sub_size),
        out_shape=[hid, hid, land, land] + expert_shapes(num_dev, exp_local, cap_slots, dim),
        in_specs=[ANY] * 6 + [vmem] * 3,
        out_specs=[vmem] * 2 + [ANY] * 4,
        scratch_shapes=[
            act_scratch(num_dev, cap_slots, ff),
            pltpu.VMEM((2, sub_size + 1, tok_count, dim), jnp.float32),
            pltpu.VMEM((sub_size, tok_count, dim), jnp.float32),
            pltpu.VMEM((3 * tok_count, 4 * room), jnp.bfloat16),
            pltpu.VMEM((4, exp_local, cap_slots, dim // PARTS), jnp.bfloat16),
            dma(2, sub_size, 4, PARTS), dma(2, sub_size, 3, PARTS), dma(2, sub_size + 1, PARTS), dma(2, sub_size, PARTS), dma(4),
        ],
        compiler_params=pltpu.CompilerParams(collective_id=collective_id, has_side_effects=True, vmem_limit_bytes=63 * 1024 * 1024),
        name='second_experts',
    )(e_a, gath_b, metas, w1, w3, w2, metas, hid_a, hid_b)


def solution(mesh):
    ep_size = mesh.shape['ep']
    sub_size = mesh.shape['sub']
    num_dev = ep_size * sub_size
    tok_spec = P(('dp', 'ep', 'sub'), None, None)
    route_spec = P(None, ('dp', 'ep', 'sub'), None)
    exp_spec = P(('ep', 'sub'), None, None)

    def device_body(input_a, input_b, route_idx, route_gate, attn_norm, w_query, w_key, w_value, w_out, moe_norm, w_gate, w_up, w_down):
        exp_local = w_gate.shape[0]
        num_exp = exp_local * num_dev
        tok_count, top_k = route_idx.shape[1:]
        dim = input_a.shape[2]
        cap_slots = 3 * top_k * tok_count // (2 * num_exp)

        meta = jnp.concatenate([jnp.stack([slot_codes(route_idx[m], num_exp, cap_slots) for m in range(2)]), route_gate], axis=2)
        meta = meta.transpose(0, 2, 1)
        hidden = [attention_block(x, attn_norm, w_query, w_key, w_value, w_out).reshape(tok_count, dim) for x in (input_a, input_b)]
        normed = [rms_norm(h, moe_norm) for h in hidden]
        gath_a, metas = gather_tokens([normed[0], meta], num_dev, sub_size, 1)
        gath_b, _, e_a = first_experts(normed[1], gath_a, metas, w_gate, w_up, w_down, cap_slots, sub_size, 2)
        outs = second_experts(e_a, gath_b, metas, w_gate, w_up, w_down, hidden[0], hidden[1], sub_size, 3)
        return outs[0].reshape(input_a.shape), outs[1].reshape(input_b.shape)

    return jax.shard_map(device_body, mesh=mesh, in_specs=(tok_spec, tok_spec, route_spec, route_spec, P(), P(), P(), P(), P(), P(), exp_spec, exp_spec, exp_spec), out_specs=(tok_spec, tok_spec), check_vma=False)
```

```python
import functools

import jax
import jax.numpy as jnp
from jax import lax
from jax.experimental import pallas as pl
from jax.experimental.pallas import tpu as pltpu
from jax.sharding import PartitionSpec as P

NORM_EPS = 1e-6
MESH = pl.DeviceIdType.MESH
VMEM_CAP = 63 * 1024 * 1024
ANY = pl.BlockSpec(memory_space=pl.ANY)


def rms_norm(values, norm_gain):
    acc_f32 = values.astype(jnp.float32)
    inv_rms = lax.rsqrt(jnp.mean(acc_f32 * acc_f32, axis=-1, keepdims=True) + NORM_EPS)
    return (acc_f32 * inv_rms * norm_gain).astype(jnp.bfloat16)


HEADS_STEP = 2


def attend(mb, q, k, v, x, w_out, gain, hid, normed, sem):
    num_heads, seq_len, head_dim = q.shape[1:]
    dim = hid.shape[1]
    load = pltpu.make_async_copy(x.at[0], hid, sem)
    load.start()

    def body(ctx):
        causal = lax.broadcasted_iota(jnp.int32, (seq_len, seq_len), 0) >= lax.broadcasted_iota(jnp.int32, (seq_len, seq_len), 1)

        def heads(indices, q_ref, k_ref, v_ref):
            n, = indices.index
            for h in range(HEADS_STEP):
                scores = lax.dot_general(q_ref[0, h], k_ref[0, h], (((1,), (1,)), ((), ())), preferred_element_type=jnp.float32) * head_dim ** -0.5
                scores = jnp.where(causal, scores, -jnp.inf)
                weights = jnp.exp(scores - jnp.max(scores, axis=-1, keepdims=True))
                prob = (weights / jnp.sum(weights, axis=-1, keepdims=True)).astype(jnp.bfloat16)
                out = jnp.dot(prob, v_ref[0, h], preferred_element_type=jnp.float32).astype(jnp.bfloat16)
                ctx[:, pl.ds(pl.multiple_of((n * HEADS_STEP + h) * head_dim, head_dim), head_dim)] = out

        spec = pl.BlockSpec((1, HEADS_STEP, seq_len, head_dim), lambda n: (mb, n, 0, 0))
        pltpu.emit_pipeline(heads, grid=(num_heads // HEADS_STEP,), in_specs=[spec] * 3, _explicit_indices=True)(q, k, v)
        load.wait()
        cut = 512

        def project(indices, w_ref):
            n, = indices.index
            cols = pl.ds(pl.multiple_of(n * cut, cut), cut)
            hid[:, cols] = (hid[:, cols].astype(jnp.float32) + jnp.dot(ctx[...], w_ref[...], preferred_element_type=jnp.float32)).astype(jnp.bfloat16)

        pltpu.emit_pipeline(project, grid=(dim // cut,), in_specs=[pl.BlockSpec((w_out.shape[0], cut), lambda n: (0, n))], _explicit_indices=True)(w_out)
        normed[...] = rms_norm(hid[...], gain[...])

    pl.run_scoped(body, pltpu.VMEM((seq_len, num_heads * head_dim), jnp.bfloat16))


def slot_codes(exp_ids, num_exp, cap_slots):
    hits = exp_ids[:, :, None] == jnp.arange(num_exp, dtype=jnp.int32)[None, None, :]
    chosen = jnp.any(hits, axis=1)
    tok_count = exp_ids.shape[0]
    before = lax.broadcasted_iota(jnp.int32, (tok_count, tok_count), 0) > lax.broadcasted_iota(jnp.int32, (tok_count, tok_count), 1)
    rank = jnp.dot(before.astype(jnp.bfloat16), chosen.astype(jnp.bfloat16), preferred_element_type=jnp.float32)
    rank_of = jnp.sum(jnp.where(hits, rank[:, None, :], 0.0), axis=2)
    return exp_ids.astype(jnp.float32) * cap_slots + rank_of


def greet(sub, sub_size, peers, to_left, to_right):
    barrier = pltpu.get_barrier_semaphore()
    last = sub_size - 1

    def hello(dev):
        pl.semaphore_signal(barrier, inc=1, device_id=dev, device_id_type=MESH)

    for dev in peers:
        hello(dev)
    pl.when(sub > 0)(lambda: hello(to_left))
    pl.when(sub < last)(lambda: hello(to_right))
    pl.semaphore_wait(barrier, len(peers) + (sub + last) // sub_size + (2 * last - sub) // sub_size)


def at_rank(sub, k):
    side = sub // 2
    near = sub + side * (3 - 2 * sub)
    a = k + near * (1 - k // 2) * (1 - 2 * k)
    return a + side * (3 - 2 * a)


def rank_of(sub, place):
    side = sub // 2
    near = sub + side * (3 - 2 * sub)
    a = place + side * (3 - 2 * place)
    return a + near * (1 - a // 2) * (1 - 2 * a)


class Gather:
    def __init__(self, sub_size, ins, outs, stage, recv, right_s, left_s, far_s, core_s, loc):
        self.count, self.sub_size = len(ins), sub_size
        self.ins, self.outs, self.stage = ins, outs, stage
        self.recv, self.right_s, self.left_s, self.far_s, self.core_s, self.loc = recv, right_s, left_s, far_s, core_s, loc
        ep, sub = lax.axis_index('ep'), lax.axis_index('sub')
        self.ep, self.sub, self.last = ep, sub, sub_size - 1
        self.ep_far = lax.rem(ep + 2, 4)
        self.ep_core = ep + 1 - 2 * lax.rem(ep, 2)
        self.ep_diag = lax.rem(self.ep_core + 2, 4)
        self.me = ep * sub_size + sub
        self.to_right, self.to_left = {'ep': ep, 'sub': sub + 1}, {'ep': ep, 'sub': sub - 1}
        self.to_far, self.to_core = {'ep': self.ep_far, 'sub': sub}, {'ep': self.ep_core, 'sub': sub}

    def copies(self, src, blk, sem, slot, dev):
        return [pltpu.make_async_remote_copy(src_ref=src(a), dst_ref=self.outs[a].at[blk], send_sem=sem.at[a, slot], recv_sem=self.recv.at[a, blk], device_id=dev, device_id_type=MESH) for a in range(self.count)]

    def start(self, *args):
        for cp in self.copies(*args):
            cp.start()

    def landed(self, blk):
        for cp in self.copies(lambda a: self.outs[a].at[blk], blk, self.far_s, 0, self.to_far):
            cp.wait_recv()

    def sent(self, sem, slot, dev):
        for cp in self.copies(lambda a: self.outs[a].at[self.me], 0, sem, slot, dev):
            cp.wait_send()

    def begin(self):
        sub, me = self.sub, self.me
        own = lambda a: self.outs[a].at[me]
        for a in range(self.count):
            if self.ins[a] is not None:
                cp = pltpu.make_async_copy(self.ins[a], self.stage[a], self.loc.at[a])
                cp.start()
                cp.wait()
        keep = [pltpu.make_async_copy(self.stage[a], own(a), self.loc.at[a]) for a in range(self.count)]
        for cp in keep:
            cp.start()
        for cp in keep:
            cp.wait()
        pl.when(sub < self.last)(lambda: self.start(own, me, self.right_s, sub, self.to_right))
        pl.when(sub > 0)(lambda: self.start(own, me, self.left_s, sub, self.to_left))
        self.start(own, me, self.far_s, sub, self.to_far)
        self.start(own, me, self.core_s, sub, self.to_core)

    def from_far(self, src_sub):
        blk = self.ep_far * self.sub_size + src_sub
        self.landed(blk)
        self.start(lambda a: self.outs[a].at[blk], blk, self.core_s, self.sub_size + src_sub, self.to_core)

    def from_line(self, src_sub, sem, cond, dev):
        blk = self.ep * self.sub_size + src_sub
        src = lambda a: self.outs[a].at[blk]
        self.landed(blk)
        pl.when(cond)(lambda: self.start(src, blk, sem, src_sub, dev))
        self.start(src, blk, self.far_s, src_sub, self.to_far)
        self.start(src, blk, self.core_s, src_sub, self.to_core)

    def hop(self, dist):
        sub, last = self.sub, self.last
        pl.when(sub - dist >= 0)(lambda: self.from_line(sub - dist, self.right_s, sub < last, self.to_right))
        pl.when(sub + dist <= last)(lambda: self.from_line(sub + dist, self.left_s, sub > 0, self.to_left))
        if dist == 1:
            self.from_far(sub)
        else:
            pl.when(sub - dist + 1 >= 0)(lambda: self.from_far(sub - dist + 1))
            pl.when(sub + dist - 1 <= last)(lambda: self.from_far(sub + dist - 1))

    def core_ready(self, first, stop):
        for k in range(first, stop):
            src_sub = at_rank(self.sub, k)
            self.landed(self.ep_core * self.sub_size + src_sub)
            self.landed(self.ep_diag * self.sub_size + src_sub)

    def last_far(self):
        sub, last = self.sub, self.last
        pl.when(sub - last >= 0)(lambda: self.from_far(sub - last))
        pl.when(sub + last <= last)(lambda: self.from_far(sub + last))

    def drain(self):
        sub, last, size = self.sub, self.last, self.sub_size
        for src_sub in range(size):
            self.sent(self.far_s, src_sub, self.to_far)
            self.sent(self.core_s, src_sub, self.to_core)
            self.sent(self.core_s, size + src_sub, self.to_core)
            pl.when((sub >= src_sub) & (sub < last))(lambda: self.sent(self.right_s, src_sub, self.to_right))
            pl.when((sub <= src_sub) & (sub > 0))(lambda: self.sent(self.left_s, src_sub, self.to_left))


def gather_scratch(arrays, num_dev, sub_size):
    sems = lambda n: pltpu.SemaphoreType.DMA((len(arrays), n))
    return [pltpu.VMEM(a.shape, a.dtype) for a in arrays] + [sems(num_dev), sems(sub_size), sems(sub_size), sems(sub_size), sems(2 * sub_size), pltpu.SemaphoreType.DMA((len(arrays),))]


FFN_STEPS = 4


HALVES = 2


def pick_rows(mb, half, ep, sub, sub_size, gath, metas, rows, exp_local, cap_slots):
    num_dev, tok_count, dim = gath.shape
    top_k = metas.shape[2] // 2
    room = exp_local * cap_slots
    blocks = num_dev // HALVES
    ep_size = num_dev // sub_size
    base = ((ep * sub_size + sub) * room).astype(jnp.float32)

    def block(p):
        q = half * blocks + p
        return (q % ep_size) * sub_size + at_rank(sub, q // ep_size)

    def pick(code_ref, tok_ref, out_ref):
        want = lax.broadcasted_iota(jnp.int32, (room, tok_count), 0).astype(jnp.float32) + base
        hit = code_ref[0, 0, 0:1, :] == want
        for j in range(1, top_k):
            hit = hit | (code_ref[0, 0, j:j + 1, :] == want)
        onehot = jnp.where(hit, 1.0, 0.0).astype(jnp.bfloat16)
        picked = jnp.dot(onehot, tok_ref[0], preferred_element_type=jnp.float32).astype(jnp.bfloat16)
        for e in range(exp_local):
            out_ref[e] = picked[e * cap_slots:(e + 1) * cap_slots]

    pltpu.emit_pipeline(
        pick,
        grid=(blocks,),
        in_specs=[pl.BlockSpec((1, 1) + metas.shape[2:], lambda p: (block(p), mb, 0, 0)), pl.BlockSpec((1, tok_count, dim), lambda p: (block(p), 0, 0))],
        out_specs=[pl.BlockSpec((exp_local, cap_slots, dim), lambda p: (0, half * blocks + p, 0))],
    )(metas, gath, rows)


def run_experts(w1, w3, w2, rows, e_out, act_ref, hook):
    num_dev, exp_local, cap_slots, dim = e_out.shape
    ff = w1.shape[2]
    steps = FFN_STEPS
    ft, nt = ff // steps, dim // steps

    def ffn(indices, x_ref, w1_ref, w3_ref, w2_ref, out_ref):
        e, step = indices.index

        @pl.when(step < steps)
        def _():
            x = x_ref[0]
            gate_h = jnp.dot(x, w1_ref[0], preferred_element_type=jnp.float32)
            up_h = jnp.dot(x, w3_ref[0], preferred_element_type=jnp.float32)
            act_ref[step] = (jax.nn.silu(gate_h) * up_h).astype(jnp.bfloat16)

        @pl.when(step >= steps)
        def _():
            acc = jnp.dot(act_ref[0], w2_ref[0, 0:ft, :], preferred_element_type=jnp.float32)
            for k in range(1, steps):
                acc = acc + jnp.dot(act_ref[k], w2_ref[0, k * ft:(k + 1) * ft, :], preferred_element_type=jnp.float32)
            out_ref[...] = acc.astype(jnp.bfloat16).reshape(out_ref.shape)

        hook(e, step)

    pltpu.emit_pipeline(
        ffn,
        grid=(exp_local, 2 * steps),
        in_specs=[
            pl.BlockSpec((1, num_dev * cap_slots, dim), lambda e, s: (e, 0, 0)),
            pl.BlockSpec((1, dim, ft), lambda e, s: (e, 0, jnp.minimum(s, steps - 1))),
            pl.BlockSpec((1, dim, ft), lambda e, s: (e, 0, jnp.minimum(s, steps - 1))),
            pl.BlockSpec((1, ff, nt), lambda e, s: (e, 0, jnp.maximum(s - steps, 0))),
        ],
        out_specs=[pl.BlockSpec((num_dev, 1, cap_slots, nt), lambda e, s: (0, e, 0, jnp.maximum(s - steps, 0)))],
        _explicit_indices=True,
    )(rows, w1, w3, w2, e_out)


PARTS = 2


class Combine:
    def __init__(self, mb, sub_size, e_ref, metas, hid, out, land, inbox, sums, mix, tile, a_recv, a_send, z_recv, z_send, loads):
        self.mb, self.sub_size, self.last = mb, sub_size, sub_size - 1
        self.e_ref, self.metas, self.hid, self.out, self.land = e_ref, metas, hid, out, land
        self.inbox, self.sums, self.mix, self.tile = inbox, sums, mix, tile
        self.a_recv, self.a_send, self.z_recv, self.z_send, self.loads = a_recv, a_send, z_recv, z_send, loads
        ep, sub = lax.axis_index('ep'), lax.axis_index('sub')
        self.ep, self.sub = ep, sub
        ep_far = lax.rem(ep + 2, 4)
        ep_core = ep + 1 - 2 * lax.rem(ep, 2)
        self.peers = [ep_far, lax.rem(ep_core + 2, 4), ep_core]
        self.to_right, self.to_left = {'ep': ep, 'sub': sub + 1}, {'ep': ep, 'sub': sub - 1}
        self.width = e_ref.shape[3] // PARTS

    def greet(self):
        greet(self.sub, self.sub_size, [{'ep': p, 'sub': self.sub} for p in self.peers], self.to_left, self.to_right)

    def order(self, i):
        side = self.sub // 2
        near = self.sub + side * (3 - 2 * self.sub)
        a = 3 - i + near * (3 * (i // 2) - 2 * ((i + 2) // 3))
        return a + side * (3 - 2 * a)

    def part(self, h):
        return pl.ds(pl.multiple_of(h * self.width, self.width), self.width)

    def slot_copy(self, dst, k, h, src_ep):
        return pltpu.make_async_remote_copy(
            src_ref=self.e_ref.at[rank_of(self.sub, dst) * 4 + self.peers[k], :, :, self.part(h)], dst_ref=self.land.at[dst, src_ep, :, :, self.part(h)],
            send_sem=self.a_send.at[self.mb, dst, k, h], recv_sem=self.a_recv.at[self.mb, dst, src_ep, h], device_id={'ep': self.peers[k], 'sub': self.sub}, device_id_type=MESH)

    def line_copy(self, dst, h, box, dev):
        return pltpu.make_async_remote_copy(
            src_ref=self.sums.at[dst, :, self.part(h)], dst_ref=self.inbox.at[self.mb, box, :, self.part(h)],
            send_sem=self.z_send.at[self.mb, dst, h], recv_sem=self.z_recv.at[self.mb, box, h], device_id=dev, device_id_type=MESH)

    def begin(self):
        @pl.loop(0, self.sub_size * PARTS)
        def _(t):
            dst = self.order(t // PARTS)
            for k in range(3):
                self.slot_copy(dst, k, t % PARTS, self.ep).start()

    def build_mix(self, dst):
        tok_count, room = self.sums.shape[1], self.e_ref.shape[1] * self.e_ref.shape[2]
        cols = lax.broadcasted_iota(jnp.int32, (tok_count, 4 * room), 1)
        want = (cols + (cols // room) * ((self.sub_size - 1) * room) + self.sub * room).astype(jnp.float32)
        route = self.metas[dst, self.mb].T
        top_k = route.shape[1] // 2
        mat = jnp.zeros((tok_count, 4 * room), jnp.float32)
        for j in range(top_k):
            mat = jnp.where(route[:, j:j + 1] == want, route[:, top_k + j:top_k + j + 1], mat)
        for s in range(3):
            piece = mat.astype(jnp.bfloat16)
            self.mix[s * tok_count:(s + 1) * tok_count, :] = piece
            mat = mat - piece.astype(jnp.float32)

    def event(self, t):
        i, h = t // PARTS, t % PARTS
        dst, sub, last = self.order(i), self.sub, self.last
        tok_count = self.sums.shape[1]
        pl.when(h == 0)(lambda: self.build_mix(dst))
        for k in range(3):
            self.slot_copy(dst, k, h, self.peers[k]).wait_recv()
        pulls = [pltpu.make_async_copy(self.land.at[dst, p, :, :, self.part(h)], self.tile.at[p], self.loads.at[p]) for p in self.peers]
        pulls.append(pltpu.make_async_copy(self.e_ref.at[rank_of(self.sub, dst) * 4 + self.ep, :, :, self.part(h)], self.tile.at[self.ep], self.loads.at[self.ep]))
        for cp in pulls:
            cp.start()
        for cp in pulls:
            cp.wait()
        cut = 256

        @pl.loop(0, self.width // cut)
        def _(c):
            rows = self.tile[:, :, :, pl.ds(pl.multiple_of(c * cut, cut), cut)].reshape(self.mix.shape[1], cut)
            prod = jnp.dot(self.mix[...], rows, preferred_element_type=jnp.float32)
            self.sums[dst, :, pl.ds(pl.multiple_of(h * self.width + c * cut, cut), cut)] = prod[0:tok_count] + (prod[tok_count:2 * tok_count] + prod[2 * tok_count:])

        def add(box):
            self.line_copy(dst, h, box, self.to_left).wait_recv()
            self.sums[dst, :, self.part(h)] = self.sums[dst, :, self.part(h)] + self.inbox[self.mb, box, :, self.part(h)]

        size = self.sub_size
        pl.when((dst >= sub) & (sub > 0))(lambda: add(dst))
        pl.when((dst <= sub) & (sub < last))(lambda: add(dst + (1 - (sub - dst + last) // size) * (size - dst)))
        pl.when(dst > sub)(lambda: self.line_copy(dst, h, dst, self.to_right).start())
        pl.when(dst < sub)(lambda: self.line_copy(dst, h, dst + (1 - (sub - 1 - dst + last) // size) * (size - dst), self.to_left).start())

        @pl.when(dst == sub)
        def _():
            self.out[:, self.part(h)] = (self.hid[:, self.part(h)].astype(jnp.float32) + self.sums[dst, :, self.part(h)]).astype(jnp.bfloat16)

    def end(self):
        @pl.loop(0, self.sub_size * PARTS)
        def _(t):
            h = t % PARTS
            dst = self.order(t // PARTS)
            for k in range(3):
                self.slot_copy(dst, k, h, self.ep).wait_send()
            pl.when(dst != self.sub)(lambda: self.line_copy(dst, h, dst, self.to_right).wait_send())


def layer_body(sub_size, q, k, v, x_a, x_b, w_out, meta, w1, w3, w2, gain, out_a, out_b, gath_a, gath_b, metas, rows_a, rows_b, e_a, e_b, land_a, land_b,
               act_ref, near_meta, hid_a, hid_b, x_sem, inbox, sums, mix, tile, meta_sem, a_recv, a_send, z_recv, z_send, loads, stage_a, stage_m, *rest):
    sems_a, stage_b, sems_b = rest[:6], rest[6], rest[7:]
    ga = Gather(sub_size, [None, meta], [gath_a, metas], [stage_a, stage_m], *sems_a)
    gb = Gather(sub_size, [None], [gath_b], [stage_b], *sems_b)
    sems = (a_recv, a_send, z_recv, z_send, loads)
    ca = Combine(0, sub_size, e_a, near_meta, hid_a, out_a, land_a, inbox, sums, mix, tile, *sems)
    cb = Combine(1, sub_size, e_b, near_meta, hid_b, out_b, land_b, inbox, sums, mix, tile, *sems)
    ep, sub = ca.ep, ca.sub
    weights = (w1, w3, w2)
    events = sub_size * PARTS

    def at(e, step, when_e, when_step, fn):
        pl.when((e == when_e) & (step == when_step))(fn)

    def pick(mb, half):
        pick_rows(mb, half, ep, sub, sub_size, (gath_a, gath_b)[mb], metas, (rows_a, rows_b)[mb], w1.shape[0], e_a.shape[2])

    def hook_a(e, step):
        at(e, step, 0, 0, lambda: gb.hop(2))
        at(e, step, 1, 4, lambda: gb.hop(3))

    def hook_b(e, step):
        pl.when(step == 2 * FFN_STEPS - 1)(lambda: ca.event(e + 1))

    ca.greet()
    attend(0, q, k, v, x_a, w_out, gain, hid_a, stage_a, x_sem)
    ga.begin()
    attend(1, q, k, v, x_b, w_out, gain, hid_b, stage_b, x_sem)
    ga.hop(1)
    ga.hop(2)
    ga.core_ready(0, 2)
    pick(0, 0)
    ga.hop(3)
    gb.begin()
    ga.last_far()
    ga.core_ready(2, 4)
    gb.hop(1)
    pick(0, 1)
    run_experts(*weights, rows_a, e_a, act_ref, hook_a)
    ca.begin()
    pull = pltpu.make_async_copy(metas.at[pl.ds(ep * sub_size, sub_size)], near_meta, meta_sem)
    pull.start()
    pull.wait()
    gb.core_ready(0, 2)
    pick(1, 0)
    gb.last_far()
    gb.core_ready(2, 4)
    pick(1, 1)
    ca.event(0)
    run_experts(*weights, rows_b, e_b, act_ref, hook_b)
    cb.begin()
    pl.loop(w1.shape[0] + 1, events)(ca.event)
    ca.end()
    pl.loop(0, events)(cb.event)
    cb.end()
    ga.drain()
    gb.drain()


def run_layer(q, k, v, x_a, x_b, w_out, meta, w1, w3, w2, gain, num_dev, cap_slots, sub_size):
    _, tok_count, dim = x_a.shape
    exp_local, _, ff = w1.shape
    room = exp_local * cap_slots
    dma = lambda *s: pltpu.SemaphoreType.DMA(s)
    bf = lambda *s: jax.ShapeDtypeStruct(s, jnp.bfloat16)
    hid, gath = bf(tok_count, dim), bf(num_dev, tok_count, dim)
    land = bf(sub_size, 4, exp_local, cap_slots, dim)
    rows, e_out = bf(exp_local, num_dev * cap_slots, dim), bf(num_dev, exp_local, cap_slots, dim)
    vmem = pl.BlockSpec(memory_space=pltpu.VMEM)
    return pl.pallas_call(
        functools.partial(layer_body, sub_size),
        out_shape=[hid, hid, gath, gath, jax.ShapeDtypeStruct((num_dev,) + meta.shape, meta.dtype), rows, rows, e_out, e_out, land, land],
        in_specs=[ANY] * 10 + [vmem],
        out_specs=[vmem] * 2 + [ANY] * 9,
        scratch_shapes=[
            pltpu.VMEM((FFN_STEPS, num_dev * cap_slots, ff // FFN_STEPS), jnp.bfloat16),
            pltpu.VMEM((sub_size,) + meta.shape, meta.dtype),
            pltpu.VMEM((tok_count, dim), jnp.bfloat16),
            pltpu.VMEM((tok_count, dim), jnp.bfloat16),
            pltpu.SemaphoreType.DMA,
            pltpu.VMEM((2, sub_size + 1, tok_count, dim), jnp.float32),
            pltpu.VMEM((sub_size, tok_count, dim), jnp.float32),
            pltpu.VMEM((3 * tok_count, 4 * room), jnp.bfloat16),
            pltpu.VMEM((4, exp_local, cap_slots, dim // PARTS), jnp.bfloat16),
            pltpu.SemaphoreType.DMA,
            dma(2, sub_size, 4, PARTS), dma(2, sub_size, 3, PARTS), dma(2, sub_size + 1, PARTS), dma(2, sub_size, PARTS), dma(4),
        ] + gather_scratch([hid, meta], num_dev, sub_size) + gather_scratch([hid], num_dev, sub_size),
        compiler_params=pltpu.CompilerParams(collective_id=1, has_side_effects=True, vmem_limit_bytes=VMEM_CAP),
        name='run_layer',
    )(q, k, v, x_a, x_b, w_out, meta, w1, w3, w2, gain)


def solution(mesh):
    ep_size = mesh.shape['ep']
    sub_size = mesh.shape['sub']
    num_dev = ep_size * sub_size
    tok_spec = P(('dp', 'ep', 'sub'), None, None)
    route_spec = P(None, ('dp', 'ep', 'sub'), None)
    exp_spec = P(('ep', 'sub'), None, None)

    def device_body(input_a, input_b, route_idx, route_gate, attn_norm, w_query, w_key, w_value, w_out, moe_norm, w_gate, w_up, w_down):
        exp_local = w_gate.shape[0]
        num_exp = exp_local * num_dev
        tok_count, top_k = route_idx.shape[1:]
        cap_slots = 3 * top_k * tok_count // (2 * num_exp)

        meta = jnp.concatenate([jnp.stack([slot_codes(route_idx[m], num_exp, cap_slots) for m in range(2)]), route_gate], axis=2)
        meta = meta.transpose(0, 2, 1)
        normed = rms_norm(jnp.concatenate([input_a, input_b]), attn_norm)
        q, k, v = [jnp.einsum('bsd,dhc->bhsc', normed, w, preferred_element_type=jnp.float32).astype(jnp.bfloat16) for w in (w_query, w_key, w_value)]
        outs = run_layer(q, k, v, input_a, input_b, w_out.reshape(-1, w_out.shape[2]), meta, w_gate, w_up, w_down, moe_norm[None, :], num_dev, cap_slots, sub_size)
        return outs[0].reshape(input_a.shape), outs[1].reshape(input_b.shape)

    return jax.shard_map(device_body, mesh=mesh, in_specs=(tok_spec, tok_spec, route_spec, route_spec, P(), P(), P(), P(), P(), P(), exp_spec, exp_spec, exp_spec), out_specs=(tok_spec, tok_spec), check_vma=False)
```

```python
import functools

import jax
import jax.numpy as jnp
from jax import lax
from jax.experimental import pallas as pl
from jax.experimental.pallas import tpu as pltpu
from jax.sharding import PartitionSpec as P

NORM_EPS = 1e-6
MESH = pl.DeviceIdType.MESH
VMEM_CAP = 63 * 1024 * 1024
ANY = pl.BlockSpec(memory_space=pl.ANY)


def rms_norm(values, norm_gain):
    acc_f32 = values.astype(jnp.float32)
    inv_rms = lax.rsqrt(jnp.mean(acc_f32 * acc_f32, axis=-1, keepdims=True) + NORM_EPS)
    return (acc_f32 * inv_rms * norm_gain).astype(jnp.bfloat16)


HEADS_STEP = 2


def attend(mb, q, k, v, x, w_out, gain, hid, normed, sem):
    num_heads, seq_len, head_dim = q.shape[1:]
    dim = hid.shape[1]
    load = pltpu.make_async_copy(x.at[0], hid, sem)
    load.start()

    def body(ctx):
        causal = lax.broadcasted_iota(jnp.int32, (seq_len, seq_len), 0) >= lax.broadcasted_iota(jnp.int32, (seq_len, seq_len), 1)

        def heads(indices, q_ref, k_ref, v_ref):
            n, = indices.index
            for h in range(HEADS_STEP):
                scores = lax.dot_general(q_ref[0, h], k_ref[0, h], (((1,), (1,)), ((), ())), preferred_element_type=jnp.float32) * head_dim ** -0.5
                scores = jnp.where(causal, scores, -jnp.inf)
                weights = jnp.exp(scores - jnp.max(scores, axis=-1, keepdims=True))
                prob = (weights / jnp.sum(weights, axis=-1, keepdims=True)).astype(jnp.bfloat16)
                out = jnp.dot(prob, v_ref[0, h], preferred_element_type=jnp.float32).astype(jnp.bfloat16)
                ctx[:, pl.ds(pl.multiple_of((n * HEADS_STEP + h) * head_dim, head_dim), head_dim)] = out

        spec = pl.BlockSpec((1, HEADS_STEP, seq_len, head_dim), lambda n: (mb, n, 0, 0))
        pltpu.emit_pipeline(heads, grid=(num_heads // HEADS_STEP,), in_specs=[spec] * 3, _explicit_indices=True)(q, k, v)
        load.wait()
        cut = 512

        def project(indices, w_ref):
            n, = indices.index
            cols = pl.ds(pl.multiple_of(n * cut, cut), cut)
            hid[:, cols] = (hid[:, cols].astype(jnp.float32) + jnp.dot(ctx[...], w_ref[...], preferred_element_type=jnp.float32)).astype(jnp.bfloat16)

        pltpu.emit_pipeline(project, grid=(dim // cut,), in_specs=[pl.BlockSpec((w_out.shape[0], cut), lambda n: (0, n))], _explicit_indices=True)(w_out)
        normed[...] = rms_norm(hid[...], gain[...])

    pl.run_scoped(body, pltpu.VMEM((seq_len, num_heads * head_dim), jnp.bfloat16))


def slot_codes(exp_ids, num_exp, cap_slots):
    hits = exp_ids[:, :, None] == jnp.arange(num_exp, dtype=jnp.int32)[None, None, :]
    chosen = jnp.any(hits, axis=1)
    tok_count = exp_ids.shape[0]
    before = lax.broadcasted_iota(jnp.int32, (tok_count, tok_count), 0) > lax.broadcasted_iota(jnp.int32, (tok_count, tok_count), 1)
    rank = jnp.dot(before.astype(jnp.bfloat16), chosen.astype(jnp.bfloat16), preferred_element_type=jnp.float32)
    rank_of = jnp.sum(jnp.where(hits, rank[:, None, :], 0.0), axis=2)
    return exp_ids.astype(jnp.float32) * cap_slots + rank_of


def greet(sub, sub_size, peers, to_left, to_right):
    barrier = pltpu.get_barrier_semaphore()
    last = sub_size - 1

    def hello(dev):
        pl.semaphore_signal(barrier, inc=1, device_id=dev, device_id_type=MESH)

    for dev in peers:
        hello(dev)
    pl.when(sub > 0)(lambda: hello(to_left))
    pl.when(sub < last)(lambda: hello(to_right))
    pl.semaphore_wait(barrier, len(peers) + (sub + last) // sub_size + (2 * last - sub) // sub_size)


def at_rank(sub, k):
    side = sub // 2
    near = sub + side * (3 - 2 * sub)
    a = k + near * (1 - k // 2) * (1 - 2 * k)
    return a + side * (3 - 2 * a)


def rank_of(sub, place):
    side = sub // 2
    near = sub + side * (3 - 2 * sub)
    a = place + side * (3 - 2 * place)
    return a + near * (1 - a // 2) * (1 - 2 * a)


class Gather:
    def __init__(self, sub_size, ins, outs, stage, entries, recv, right_s, left_s, far_s, core_s, loc):
        self.sub_size, self.entries = sub_size, entries
        self.ins, self.outs, self.stage = ins, outs, stage
        self.recv, self.right_s, self.left_s, self.far_s, self.core_s, self.loc = recv, right_s, left_s, far_s, core_s, loc
        ep, sub = lax.axis_index('ep'), lax.axis_index('sub')
        self.ep, self.sub, self.last = ep, sub, sub_size - 1
        self.ep_far = lax.rem(ep + 2, 4)
        self.ep_core = ep + 1 - 2 * lax.rem(ep, 2)
        self.ep_diag = lax.rem(self.ep_core + 2, 4)
        self.me = ep * sub_size + sub
        self.to_right, self.to_left = {'ep': ep, 'sub': sub + 1}, {'ep': ep, 'sub': sub - 1}
        self.to_far, self.to_core = {'ep': self.ep_far, 'sub': sub}, {'ep': self.ep_core, 'sub': sub}

    def copy(self, n, blk, sem, slot, dev):
        a, first, rows, _ = self.entries[n]
        ref = self.outs[a].at[blk, pl.ds(first, rows)]
        return pltpu.make_async_remote_copy(src_ref=ref, dst_ref=ref, send_sem=sem.at[n, slot], recv_sem=self.recv.at[n, blk], device_id=dev, device_id_type=MESH)

    def right(self, n, blk, slot):
        pl.when(self.sub < self.last)(lambda: self.copy(n, blk, self.right_s, slot, self.to_right).start())

    def left(self, n, blk, slot):
        pl.when(self.sub > 0)(lambda: self.copy(n, blk, self.left_s, slot, self.to_left).start())

    def each(self, fn):
        for n, entry in enumerate(self.entries):
            fn(n, entry[3] == 'far')

    def begin(self):
        sub, me = self.sub, self.me
        for a, src in enumerate(self.ins):
            if src is not None:
                cp = pltpu.make_async_copy(src, self.stage[a], self.loc.at[a])
                cp.start()
                cp.wait()
        keep = [pltpu.make_async_copy(self.stage[a], self.outs[a].at[me], self.loc.at[a]) for a in range(len(self.ins))]
        for cp in keep:
            cp.start()
        for cp in keep:
            cp.wait()

        def own(n, far):
            self.copy(n, me, self.far_s, sub, self.to_far).start()
            self.right(n, me, sub)
            self.left(n, me, sub)
            self.copy(n, me, self.core_s, sub, self.to_core).start()

        for n, entry in enumerate(self.entries):
            if entry[3] == 'far':
                own(n, True)
        for n, entry in enumerate(self.entries):
            if entry[3] == 'line':
                own(n, False)

    def from_near(self, src_sub, send):
        blk = self.ep * self.sub_size + src_sub

        def one(n, far):
            self.copy(n, blk, self.far_s, 0, self.to_far).wait_recv()
            send(n, blk, src_sub)
            if not far:
                self.copy(n, blk, self.far_s, src_sub, self.to_far).start()
            self.copy(n, blk, self.core_s, src_sub, self.to_core).start()

        self.each(one)

    def from_far(self, src_sub, sends):
        blk = self.ep_far * self.sub_size + src_sub
        slot = self.sub_size + src_sub

        def one(n, far):
            self.copy(n, blk, self.far_s, 0, self.to_far).wait_recv()
            if far:
                for send in sends:
                    send(n, blk, slot)
            self.copy(n, blk, self.core_s, slot, self.to_core).start()

        self.each(one)

    def far_pair(self, dist):
        sub, last = self.sub, self.last
        pl.when(sub - dist >= 0)(lambda: self.from_far(sub - dist, [self.right]))
        pl.when(sub + dist <= last)(lambda: self.from_far(sub + dist, [self.left]))

    def hop(self, dist):
        sub, last = self.sub, self.last
        pl.when(sub - dist >= 0)(lambda: self.from_near(sub - dist, self.right))
        pl.when(sub + dist <= last)(lambda: self.from_near(sub + dist, self.left))
        if dist == 1:
            self.from_far(sub, [self.right, self.left])
        else:
            self.far_pair(dist - 1)

    def core_ready(self, first, stop):
        for k in range(first, stop):
            src_sub = at_rank(self.sub, k)
            for ep in (self.ep_core, self.ep_diag):
                self.each(lambda n, far: self.copy(n, ep * self.sub_size + src_sub, self.far_s, 0, self.to_far).wait_recv())

    def last_far(self):
        self.far_pair(self.last)

    def drain(self):
        sub, last, size = self.sub, self.last, self.sub_size

        def one(n, far):
            sent = lambda sem, slot: self.copy(n, 0, sem, slot, self.to_far).wait_send()
            for src in range(size):
                sent(self.core_s, src)
                sent(self.core_s, size + src)
                if not far:
                    sent(self.far_s, src)
                for slot in ((src, size + src) if far else (src,)):
                    pl.when((sub >= src) & (sub < last))(lambda: sent(self.right_s, slot))
                    pl.when((sub <= src) & (sub > 0))(lambda: sent(self.left_s, slot))
            if far:
                sent(self.far_s, sub)

        self.each(one)


def gather_scratch(arrays, entries, num_dev, sub_size):
    sems = lambda n: pltpu.SemaphoreType.DMA((len(entries), n))
    return [pltpu.VMEM(a.shape, a.dtype) for a in arrays] + [sems(num_dev)] + [sems(2 * sub_size) for _ in range(4)] + [pltpu.SemaphoreType.DMA((len(arrays),))]


def split_rows(rows, first_far):
    return [(0, 0, first_far, 'line'), (0, first_far, rows - first_far, 'far')]


FFN_STEPS = 4
SPLIT = 1
LINE_ROWS_A = 208
LINE_ROWS_B = 208


def pick_rows(mb, first, ranks, ep, sub, sub_size, gath, metas, rows, exp_local, cap_slots):
    num_dev, tok_count, dim = gath.shape
    top_k = metas.shape[2] // 2
    room = exp_local * cap_slots
    ep_size = num_dev // sub_size
    blocks = ranks * ep_size
    base = ((ep * sub_size + sub) * room).astype(jnp.float32)

    def block(p):
        q = first * ep_size + p
        return (q % ep_size) * sub_size + at_rank(sub, q // ep_size)

    def pick(code_ref, tok_ref, out_ref):
        want = lax.broadcasted_iota(jnp.int32, (room, tok_count), 0).astype(jnp.float32) + base
        hit = code_ref[0, 0, 0:1, :] == want
        for j in range(1, top_k):
            hit = hit | (code_ref[0, 0, j:j + 1, :] == want)
        onehot = jnp.where(hit, 1.0, 0.0).astype(jnp.bfloat16)
        picked = jnp.dot(onehot, tok_ref[0], preferred_element_type=jnp.float32).astype(jnp.bfloat16)
        for e in range(exp_local):
            out_ref[e] = picked[e * cap_slots:(e + 1) * cap_slots]

    pltpu.emit_pipeline(
        pick,
        grid=(blocks,),
        in_specs=[pl.BlockSpec((1, 1) + metas.shape[2:], lambda p: (block(p), mb, 0, 0)), pl.BlockSpec((1, tok_count, dim), lambda p: (block(p), 0, 0))],
        out_specs=[pl.BlockSpec((exp_local, cap_slots, dim), lambda p: (0, first * ep_size + p, 0))],
    )(metas, gath, rows)


def run_experts(w1, w3, w2, rows, e_out, act_ref, hook):
    num_dev, exp_local, cap_slots, dim = e_out.shape
    ff = w1.shape[2]
    steps = FFN_STEPS
    ft, nt = ff // steps, dim // steps

    def ffn(indices, x_ref, w1_ref, w3_ref, w2_ref, out_ref):
        e, step = indices.index

        @pl.when(step < steps)
        def _():
            cols = pl.ds(pl.multiple_of(step * ft, ft), ft)
            for m in range(SPLIT):
                part = pl.ds(m * (act_ref.shape[0] // SPLIT), act_ref.shape[0] // SPLIT)
                x = x_ref[0, part, :]
                gate_h = jnp.dot(x, w1_ref[0], preferred_element_type=jnp.float32)
                up_h = jnp.dot(x, w3_ref[0], preferred_element_type=jnp.float32)
                act_ref[part, cols] = (jax.nn.silu(gate_h) * up_h).astype(jnp.bfloat16)

        @pl.when(step >= steps)
        def _():
            acc = jnp.dot(act_ref[...], w2_ref[0], preferred_element_type=jnp.float32)
            out_ref[...] = acc.astype(jnp.bfloat16).reshape(out_ref.shape)

        hook(e, step)

    pltpu.emit_pipeline(
        ffn,
        grid=(exp_local, 2 * steps),
        in_specs=[
            pl.BlockSpec((1, num_dev * cap_slots, dim), lambda e, s: (e, 0, 0)),
            pl.BlockSpec((1, dim, ft), lambda e, s: (e, 0, jnp.minimum(s, steps - 1))),
            pl.BlockSpec((1, dim, ft), lambda e, s: (e, 0, jnp.minimum(s, steps - 1))),
            pl.BlockSpec((1, ff, nt), lambda e, s: (e, 0, jnp.maximum(s - steps, 0))),
        ],
        out_specs=[pl.BlockSpec((num_dev, 1, cap_slots, nt), lambda e, s: (0, e, 0, jnp.maximum(s - steps, 0)))],
        _explicit_indices=True,
    )(rows, w1, w3, w2, e_out)


PARTS = 4


class Combine:
    def __init__(self, mb, sub_size, e_ref, metas, hid, out, land, inbox, sums, mix, tile, a_recv, a_send, z_recv, z_send, loads):
        self.mb, self.sub_size, self.last = mb, sub_size, sub_size - 1
        self.e_ref, self.metas, self.hid, self.out, self.land = e_ref, metas, hid, out, land
        self.inbox, self.sums, self.mix, self.tile = inbox, sums, mix, tile
        self.a_recv, self.a_send, self.z_recv, self.z_send, self.loads = a_recv, a_send, z_recv, z_send, loads
        ep, sub = lax.axis_index('ep'), lax.axis_index('sub')
        self.ep, self.sub = ep, sub
        ep_far = lax.rem(ep + 2, 4)
        ep_core = ep + 1 - 2 * lax.rem(ep, 2)
        self.peers = [ep_far, lax.rem(ep_core + 2, 4), ep_core]
        self.to_right, self.to_left = {'ep': ep, 'sub': sub + 1}, {'ep': ep, 'sub': sub - 1}
        self.width = e_ref.shape[3] // PARTS

    def greet(self):
        greet(self.sub, self.sub_size, [{'ep': p, 'sub': self.sub} for p in self.peers], self.to_left, self.to_right)

    def order(self, i):
        side = self.sub // 2
        near = self.sub + side * (3 - 2 * self.sub)
        a = 3 - i + near * (3 * (i // 2) - 2 * ((i + 2) // 3))
        return a + side * (3 - 2 * a)

    def part(self, h):
        return pl.ds(pl.multiple_of(h * self.width, self.width), self.width)

    def slot_copy(self, dst, k, h, src_ep):
        return pltpu.make_async_remote_copy(
            src_ref=self.e_ref.at[rank_of(self.sub, dst) * 4 + self.peers[k], :, :, self.part(h)], dst_ref=self.land.at[dst, src_ep, :, :, self.part(h)],
            send_sem=self.a_send.at[self.mb, dst, k, h], recv_sem=self.a_recv.at[self.mb, dst, src_ep, h], device_id={'ep': self.peers[k], 'sub': self.sub}, device_id_type=MESH)

    def line_copy(self, dst, h, box, dev):
        return pltpu.make_async_remote_copy(
            src_ref=self.sums.at[dst, :, self.part(h)], dst_ref=self.inbox.at[self.mb, box, :, self.part(h)],
            send_sem=self.z_send.at[self.mb, dst, h], recv_sem=self.z_recv.at[self.mb, box, h], device_id=dev, device_id_type=MESH)

    def begin(self):
        @pl.loop(0, self.sub_size * PARTS)
        def _(t):
            dst = self.order(t // PARTS)
            for k in range(3):
                self.slot_copy(dst, k, t % PARTS, self.ep).start()

    def build_mix(self, dst):
        tok_count, room = self.sums.shape[1], self.e_ref.shape[1] * self.e_ref.shape[2]
        cols = lax.broadcasted_iota(jnp.int32, (tok_count, 4 * room), 1)
        want = (cols + (cols // room) * ((self.sub_size - 1) * room) + self.sub * room).astype(jnp.float32)
        route = self.metas[dst, self.mb].T
        top_k = route.shape[1] // 2
        mat = jnp.zeros((tok_count, 4 * room), jnp.float32)
        for j in range(top_k):
            mat = jnp.where(route[:, j:j + 1] == want, route[:, top_k + j:top_k + j + 1], mat)
        for s in range(3):
            piece = mat.astype(jnp.bfloat16)
            self.mix[s * tok_count:(s + 1) * tok_count, :] = piece
            mat = mat - piece.astype(jnp.float32)

    def event(self, t):
        i, h = t // PARTS, t % PARTS
        dst, sub, last = self.order(i), self.sub, self.last
        tok_count = self.sums.shape[1]
        pl.when(h == 0)(lambda: self.build_mix(dst))
        for k in range(3):
            self.slot_copy(dst, k, h, self.peers[k]).wait_recv()
        pulls = [pltpu.make_async_copy(self.land.at[dst, p, :, :, self.part(h)], self.tile.at[p], self.loads.at[p]) for p in self.peers]
        pulls.append(pltpu.make_async_copy(self.e_ref.at[rank_of(self.sub, dst) * 4 + self.ep, :, :, self.part(h)], self.tile.at[self.ep], self.loads.at[self.ep]))
        for cp in pulls:
            cp.start()
        for cp in pulls:
            cp.wait()
        cut = 256

        @pl.loop(0, self.width // cut)
        def _(c):
            rows = self.tile[:, :, :, pl.ds(pl.multiple_of(c * cut, cut), cut)].reshape(self.mix.shape[1], cut)
            prod = jnp.dot(self.mix[...], rows, preferred_element_type=jnp.float32)
            self.sums[dst, :, pl.ds(pl.multiple_of(h * self.width + c * cut, cut), cut)] = prod[0:tok_count] + (prod[tok_count:2 * tok_count] + prod[2 * tok_count:])

        def add(box):
            self.line_copy(dst, h, box, self.to_left).wait_recv()
            self.sums[dst, :, self.part(h)] = self.sums[dst, :, self.part(h)] + self.inbox[self.mb, box, :, self.part(h)]

        size = self.sub_size
        pl.when((dst >= sub) & (sub > 0))(lambda: add(dst))
        pl.when((dst <= sub) & (sub < last))(lambda: add(dst + (1 - (sub - dst + last) // size) * (size - dst)))
        pl.when(dst > sub)(lambda: self.line_copy(dst, h, dst, self.to_right).start())
        pl.when(dst < sub)(lambda: self.line_copy(dst, h, dst + (1 - (sub - 1 - dst + last) // size) * (size - dst), self.to_left).start())

        @pl.when(dst == sub)
        def _():
            self.out[:, self.part(h)] = (self.hid[:, self.part(h)].astype(jnp.float32) + self.sums[dst, :, self.part(h)]).astype(jnp.bfloat16)

    def end(self):
        @pl.loop(0, self.sub_size * PARTS)
        def _(t):
            h = t % PARTS
            dst = self.order(t // PARTS)
            for k in range(3):
                self.slot_copy(dst, k, h, self.ep).wait_send()
            pl.when(dst != self.sub)(lambda: self.line_copy(dst, h, dst, self.to_right).wait_send())


def layer_body(sub_size, entries_a, entries_b, q, k, v, x_a, x_b, w_out, meta, w1, w3, w2, gain, out_a, out_b, gath_a, gath_b, metas, rows_a, rows_b, e_a, e_b, land_a, land_b,
               act_ref, near_meta, hid_a, hid_b, x_sem, inbox, sums, mix, tile, meta_sem, a_recv, a_send, z_recv, z_send, loads, stage_a, stage_m, *rest):
    sems_a, stage_b, sems_b = rest[:6], rest[6], rest[7:]
    ga = Gather(sub_size, [None, meta], [gath_a, metas], [stage_a, stage_m], entries_a, *sems_a)
    gb = Gather(sub_size, [None], [gath_b], [stage_b], entries_b, *sems_b)
    sems = (a_recv, a_send, z_recv, z_send, loads)
    ca = Combine(0, sub_size, e_a, near_meta, hid_a, out_a, land_a, inbox, sums, mix, tile, *sems)
    cb = Combine(1, sub_size, e_b, near_meta, hid_b, out_b, land_b, inbox, sums, mix, tile, *sems)
    ep, sub = ca.ep, ca.sub
    weights = (w1, w3, w2)
    events = sub_size * PARTS

    def at(e, step, when_e, when_step, fn):
        pl.when((e == when_e) & (step == when_step))(fn)

    def pick(mb, first, ranks):
        pick_rows(mb, first, ranks, ep, sub, sub_size, (gath_a, gath_b)[mb], metas, (rows_a, rows_b)[mb], w1.shape[0], e_a.shape[2])

    def hook_a(e, step):
        at(e, step, 0, 7, lambda: gb.hop(2))
        at(e, step, 2, 4, lambda: gb.hop(3))

    def hook_b(e, step):
        pl.when(step % FFN_STEPS == FFN_STEPS - 1)(lambda: ca.event(2 + 2 * e + step // FFN_STEPS))

    ca.greet()
    attend(0, q, k, v, x_a, w_out, gain, hid_a, stage_a, x_sem)
    ga.begin()
    attend(1, q, k, v, x_b, w_out, gain, hid_b, stage_b, x_sem)
    ga.hop(1)
    ga.hop(2)
    ga.core_ready(0, 2)
    pick(0, 0, 2)
    ga.hop(3)
    gb.begin()
    ga.core_ready(2, 3)
    pick(0, 2, 1)
    ga.last_far()
    ga.core_ready(3, 4)
    pick(0, 3, 1)
    gb.hop(1)
    run_experts(*weights, rows_a, e_a, act_ref, hook_a)
    ca.begin()
    pull = pltpu.make_async_copy(metas.at[pl.ds(ep * sub_size, sub_size)], near_meta, meta_sem)
    pull.start()
    pull.wait()
    gb.core_ready(0, 2)
    gb.last_far()
    pick(1, 0, 2)
    ca.event(0)
    gb.core_ready(2, 4)
    pick(1, 2, 2)
    ca.event(1)
    run_experts(*weights, rows_b, e_b, act_ref, hook_b)
    cb.begin()
    pl.loop(2 + 2 * w1.shape[0], events)(ca.event)
    ca.end()
    pl.loop(0, events)(cb.event)
    cb.end()
    ga.drain()
    gb.drain()


def run_layer(q, k, v, x_a, x_b, w_out, meta, w1, w3, w2, gain, num_dev, cap_slots, sub_size):
    _, tok_count, dim = x_a.shape
    exp_local, _, ff = w1.shape
    room = exp_local * cap_slots
    dma = lambda *s: pltpu.SemaphoreType.DMA(s)
    bf = lambda *s: jax.ShapeDtypeStruct(s, jnp.bfloat16)
    hid, gath = bf(tok_count, dim), bf(num_dev, tok_count, dim)
    land = bf(sub_size, 4, exp_local, cap_slots, dim)
    rows, e_out = bf(exp_local, num_dev * cap_slots, dim), bf(num_dev, exp_local, cap_slots, dim)
    vmem = pl.BlockSpec(memory_space=pltpu.VMEM)
    entries_a = split_rows(tok_count, LINE_ROWS_A) + [(1, 0, meta.shape[0], 'line')]
    entries_b = split_rows(tok_count, LINE_ROWS_B)
    return pl.pallas_call(
        functools.partial(layer_body, sub_size, entries_a, entries_b),
        out_shape=[hid, hid, gath, gath, jax.ShapeDtypeStruct((num_dev,) + meta.shape, meta.dtype), rows, rows, e_out, e_out, land, land],
        in_specs=[ANY] * 10 + [vmem],
        out_specs=[vmem] * 2 + [ANY] * 9,
        scratch_shapes=[
            pltpu.VMEM((num_dev * cap_slots, ff), jnp.bfloat16),
            pltpu.VMEM((sub_size,) + meta.shape, meta.dtype),
            pltpu.VMEM((tok_count, dim), jnp.bfloat16),
            pltpu.VMEM((tok_count, dim), jnp.bfloat16),
            pltpu.SemaphoreType.DMA,
            pltpu.VMEM((2, sub_size + 1, tok_count, dim), jnp.float32),
            pltpu.VMEM((sub_size, tok_count, dim), jnp.float32),
            pltpu.VMEM((3 * tok_count, 4 * room), jnp.bfloat16),
            pltpu.VMEM((4, exp_local, cap_slots, dim // PARTS), jnp.bfloat16),
            pltpu.SemaphoreType.DMA,
            dma(2, sub_size, 4, PARTS), dma(2, sub_size, 3, PARTS), dma(2, sub_size + 1, PARTS), dma(2, sub_size, PARTS), dma(4),
        ] + gather_scratch([hid, meta], entries_a, num_dev, sub_size) + gather_scratch([hid], entries_b, num_dev, sub_size),
        compiler_params=pltpu.CompilerParams(collective_id=1, has_side_effects=True, vmem_limit_bytes=VMEM_CAP),
        name='run_layer',
    )(q, k, v, x_a, x_b, w_out, meta, w1, w3, w2, gain)


def solution(mesh):
    ep_size = mesh.shape['ep']
    sub_size = mesh.shape['sub']
    num_dev = ep_size * sub_size
    tok_spec = P(('dp', 'ep', 'sub'), None, None)
    route_spec = P(None, ('dp', 'ep', 'sub'), None)
    exp_spec = P(('ep', 'sub'), None, None)

    def device_body(input_a, input_b, route_idx, route_gate, attn_norm, w_query, w_key, w_value, w_out, moe_norm, w_gate, w_up, w_down):
        exp_local = w_gate.shape[0]
        num_exp = exp_local * num_dev
        tok_count, top_k = route_idx.shape[1:]
        cap_slots = 3 * top_k * tok_count // (2 * num_exp)

        meta = jnp.concatenate([jnp.stack([slot_codes(route_idx[m], num_exp, cap_slots) for m in range(2)]), route_gate], axis=2)
        meta = meta.transpose(0, 2, 1)
        normed = rms_norm(jnp.concatenate([input_a, input_b]), attn_norm)
        q, k, v = [jnp.einsum('bsd,dhc->bhsc', normed, w, preferred_element_type=jnp.float32).astype(jnp.bfloat16) for w in (w_query, w_key, w_value)]
        outs = run_layer(q, k, v, input_a, input_b, w_out.reshape(-1, w_out.shape[2]), meta, w_gate, w_up, w_down, moe_norm[None, :], num_dev, cap_slots, sub_size)
        return outs[0].reshape(input_a.shape), outs[1].reshape(input_b.shape)

    return jax.shard_map(device_body, mesh=mesh, in_specs=(tok_spec, tok_spec, route_spec, route_spec, P(), P(), P(), P(), P(), P(), exp_spec, exp_spec, exp_spec), out_specs=(tok_spec, tok_spec), check_vma=False)
```
